32 devices in a mesh: dp: 8 (over z, y), mp: 4 (over x, core).
Axes of the slice: x: 2, y: 2, z: 4, core: 2. Of those that a mesh axis runs over, the one named last changes fastest.
Arguments:
- streams: bfloat16 [2048, 4, 8192], P('dp', None, 'mp'), may hold values from -200 to 200
- branch_out: bfloat16 [2048, 8192], P('dp', 'mp'), may hold values from -6 to 6
- merge_weight: float32 [20, 4, 8192], P(None, None, ('mp', 'dp')), may hold values from -0.03125 to 0.03125
- next_weight: float32 [24, 4, 8192], P(None, None, ('mp', 'dp')), may hold values from -0.03125 to 0.03125
- blend_bias: float32 [44], replicated, may hold values from -3 to 3
- blend_scale: float32 [5], replicated, may hold values from 0.5 to 3
- norm_gain: float32 [8192], P('mp'), may hold values from 0.5 to 1.5
Outputs:
- streams_out: bfloat16 [2048, 4, 8192], P('dp', None, 'mp')
- branch_in: bfloat16 [2048, 8192], P('dp', 'mp')
- next_mix: float32 [2048, 20], P('dp')
The draws below stay inside these ranges and needn't reach their ends.
All inputs are finite; a program needn't handle non-finite values.
Results may differ from the reference program's by a relative error of at most 0.001.
Values sent between devices are 32-bit elements; how exact they have to be, the bound alone decides.
No kernel may reach another device: no remote copies, remote signals or barrier semaphores. Data moves between devices by JAX's collectives and lax.ppermute only.
A program may use at most 64 MiB of HBM per device.

```python
import math
import jax
import jax.numpy as jnp
from jax import lax

D = 8192
STREAMS = 4
BALANCE_ROUNDS = 6
TOK_DEV = 256
TOKENS = 2048
N_DP = 8


def draw_streams(key, part):
    subkeys = jax.random.split(jax.random.fold_in(key, 7), 3)
    row_scale = jnp.exp(jax.random.uniform(subkeys[0], (TOKENS, 1, 1), minval=math.log(0.3), maxval=math.log(3.0)))
    feature_ramp = jnp.arange(D, dtype=jnp.float32) / D
    col_scale = jnp.exp(jax.random.uniform(subkeys[1], (1, STREAMS, D), minval=math.log(0.3), maxval=math.log(3.0))) * 3.0 ** feature_ramp / math.sqrt(3.0)
    base_draw = jnp.clip(jax.random.normal(subkeys[2], (TOKENS, STREAMS, D)), -6.0, 6.0)
    return (base_draw * row_scale * col_scale).astype(jnp.bfloat16)


def steps_of(own_key, extent, shards, least, largest):
    def one(position, blocks):
        draws = jax.random.uniform(jax.random.fold_in(jax.random.fold_in(own_key, 6), position), (blocks,), jnp.float32, least / len(shards), largest / len(shards))
        return jnp.repeat(jnp.exp(draws), extent[position] // blocks).reshape((-1,) + (1,) * (len(extent) - position - 1))

    factor_of = one(*shards[0])
    for cut in shards[1:]:
        factor_of = factor_of * one(*cut)
    return factor_of


def noise(own_key, shape, spread, reach, shards=(), held_as=jnp.bfloat16):
    array = spread * jax.random.normal(own_key, shape, jnp.float32)
    if shards:
        array = array * steps_of(own_key, shape, shards, -0.22, 0.18)
    return jnp.clip(array, -reach, reach).astype(held_as)


def setup_inputs(seed: int = 0) -> dict:
    keys = jax.random.split(jax.random.key(seed), 8)
    return {
        "streams": draw_streams(jax.random.fold_in(keys[7], 71), 0),
        "branch_out": noise(keys[1], (TOKENS, D), 1.0, 6.0, ((0, 8), (1, 4))),
        "merge_weight": noise(keys[2], (20, STREAMS, D), (STREAMS * D) ** -0.5, 0.03125, ((2, 32),), jnp.float32),
        "next_weight": noise(keys[3], (24, STREAMS, D), (STREAMS * D) ** -0.5, 0.03125, ((2, 32),), jnp.float32),
        "blend_bias": noise(keys[4], (44,), 1.0, 3.0, (), jnp.float32),
        "blend_scale": jnp.clip(jnp.exp(jax.random.uniform(keys[5], (5,), jnp.float32, math.log(0.5), math.log(3.0))), 0.5, 3.0),
        "norm_gain": jnp.clip(1.0 + 0.1 * jax.random.normal(keys[6], (D,), jnp.float32), 0.5, 1.5),
    }


epsilon = 1e-06

def balance_normalize(balanced_matrix):
    for balance_round in range(BALANCE_ROUNDS):
        balanced_matrix = balanced_matrix / lax.optimization_barrier(jnp.sum(balanced_matrix, axis=2, keepdims=True))
        balanced_matrix = balanced_matrix / lax.optimization_barrier(jnp.sum(balanced_matrix, axis=1, keepdims=True))
    return balanced_matrix

def logits_of(widened, weight):
    squares = lax.optimization_barrier(jnp.sum(widened * widened, axis=(1, 2)))
    rms_root = jnp.sqrt(squares / (STREAMS * D) + epsilon)
    raw_part = jnp.einsum('tic,kic->tk', widened, weight, precision=lax.Precision.HIGHEST)
    return raw_part / rms_root[:, None]

def layer_block(block_streams, block_branch, merge_weight, next_weight, blend_bias, blend_scale, norm_gain):
    widened = block_streams.astype(jnp.float32)
    score_logits = logits_of(widened, merge_weight)
    post_mix = 2.0 * jax.nn.sigmoid(blend_scale[0] * score_logits[:, :4] + blend_bias[:4])
    residual_blend = balance_normalize(jnp.exp(blend_scale[1] * score_logits[:, 4:20].reshape(-1, 4, 4) + blend_bias[4:20].reshape(4, 4)))
    mixed = jnp.einsum('tji,tic->tjc', residual_blend, widened, precision=lax.Precision.HIGHEST)
    mixed = mixed + post_mix[:, :, None] * block_branch.astype(jnp.float32)[:, None, :]
    merged_out = mixed.astype(jnp.bfloat16)
    following_logits = logits_of(mixed, next_weight)
    pre_next = jax.nn.sigmoid(blend_scale[2] * following_logits[:, :4] + blend_bias[20:24])
    post_next = 2.0 * jax.nn.sigmoid(blend_scale[3] * following_logits[:, 4:8] + blend_bias[24:28])
    residual_following = balance_normalize(jnp.exp(blend_scale[4] * following_logits[:, 8:24].reshape(-1, 4, 4) + blend_bias[28:44].reshape(4, 4)))
    united = jnp.einsum('ti,tic->tc', pre_next, mixed, precision=lax.Precision.HIGHEST)
    united_sq = lax.optimization_barrier(jnp.sum(united * united, axis=1))
    branch_in = (united / jnp.sqrt(united_sq / D + epsilon)[:, None] * norm_gain).astype(jnp.bfloat16)
    next_mix = jnp.concatenate([post_next, residual_following.reshape(-1, 16)], axis=1)
    return (merged_out, branch_in, next_mix)

def reference(streams, branch_out, merge_weight, next_weight, blend_bias, blend_scale, norm_gain):
    stacked = streams.reshape(N_DP, TOK_DEV, STREAMS, D)
    branch_blocks = branch_out.reshape(N_DP, TOK_DEV, D)

    def one_block(pair):
        return layer_block(pair[0], pair[1], merge_weight, next_weight, blend_bias, blend_scale, norm_gain)
    merged_out, branch_in, next_mix = lax.map(one_block, (stacked, branch_blocks))
    return (merged_out.reshape(TOKENS, STREAMS, D), branch_in.reshape(TOKENS, D), next_mix.reshape(TOKENS, 20))
```

```python
import functools

import jax
import jax.numpy as jnp
from jax import lax
from jax.experimental import pallas as pl
from jax.experimental.pallas import tpu as pltpu
from jax.sharding import PartitionSpec as P

BALANCE_ROUNDS = 6
EPS = 1e-06
FB = 256
GT = 64
F32 = jnp.float32
BF16 = jnp.bfloat16
MIB = 2**20

VMEM = pl.BlockSpec(memory_space=pltpu.VMEM)
SMEM = pl.BlockSpec(memory_space=pltpu.SMEM)
HBM = pl.BlockSpec(memory_space=pltpu.HBM)

PAIRS = [(i, j) for i in range(4) for j in range(i, 4)]


def _nt(a, b, precision=None):
    return lax.dot_general(
        a, b, (((1,), (1,)), ((), ())), precision=precision, preferred_element_type=F32
    )


def _split(x):
    hi = x.astype(BF16)
    return hi, (x - hi.astype(F32)).astype(BF16)


def _iota(shape, dim):
    return lax.broadcasted_iota(jnp.int32, shape, dim)


def _store_by_column(ref, rows, start):
    ref[0:start, :] = rows[0:start]
    for j in range(4):
        for i in range(4):
            source = start + 4 * j + i
            ref[start + 4 * i + j : start + 4 * i + j + 1, :] = rows[source : source + 1]
    if ref.shape[0] > start + 16:
        ref[start + 16 :, :] = rows[start + 16 :]


def pre_kernel(s_hbm, b_ref, sil_ref, sde_ref, g_ref, acc_ref, sems):
    tokens, width = b_ref.shape
    tiles = width // 128
    rows = 4 * tokens
    blocks = width // FB

    def copy(c):
        return pltpu.make_async_copy(
            s_hbm.at[:, :, pl.ds(pl.multiple_of(c * 128, 128), 128)], sil_ref.at[c], sems.at[c]
        )

    for c in range(tiles):
        copy(c).start()
    r, q = _iota((4 * GT, 4 * GT), 0), _iota((4 * GT, 4 * GT), 1)
    perm = jnp.where(q == 4 * (r % GT) + r // GT, 1.0, 0.0).astype(BF16)
    acc_ref[...] = jnp.zeros_like(acc_ref)

    def body(k, _):
        copy(2 * k).wait()
        copy(2 * k + 1).wait()
        left = sil_ref.at[2 * k].reshape(rows, 128)
        right = sil_ref.at[2 * k + 1].reshape(rows, 128)
        for g in range(tokens // GT):
            own = pl.ds(g * 4 * GT, 4 * GT)
            x = jnp.concatenate([left[own, :], right[own, :]], axis=1)
            y = jnp.dot(perm, x, preferred_element_type=F32)
            for i in range(4):
                sde_ref[k, i, pl.ds(g * GT, GT), :] = y[i * GT : (i + 1) * GT].astype(BF16)

        def grams(c, _):
            at = pl.ds(pl.multiple_of(c * 16, 16), 16)
            wide = [sde_ref[k, i, at, :].astype(F32) for i in range(4)]
            lanes = pl.ds(pl.multiple_of(k * FB, FB), FB)
            wide.append(b_ref[at, lanes].astype(F32))
            products = [wide[i] * wide[j] for i, j in PAIRS]
            products += [wide[i] * wide[4] for i in range(5)]
            for p, product in enumerate(products):
                acc_ref[p, at, :] += product[:, :128] + product[:, 128:]
            return 0

        lax.fori_loop(0, tokens // 16, grams, 0)
        return 0

    lax.fori_loop(0, blocks, body, 0)
    ones = jnp.ones((8, 128), F32)
    for p in range(15):
        g_ref[p : p + 1, :] = _nt(ones, acc_ref[p], lax.Precision.HIGHEST)[0:1]
    g_ref[15:16, :] = jnp.zeros((1, tokens), F32)


def pre(streams, branch):
    tokens, _, width = streams.shape
    return pl.pallas_call(
        pre_kernel,
        out_shape=(
            jax.ShapeDtypeStruct((width // 128, tokens, 4, 128), BF16),
            jax.ShapeDtypeStruct((width // FB, 4, tokens, FB), BF16),
            jax.ShapeDtypeStruct((16, tokens), F32),
        ),
        in_specs=[HBM, VMEM],
        out_specs=(VMEM, VMEM, VMEM),
        scratch_shapes=[
            pltpu.VMEM((15, tokens, 128), F32),
            pltpu.SemaphoreType.DMA((width // 128,)),
        ],
        compiler_params=pltpu.CompilerParams(vmem_limit_bytes=20 * MIB),
        cost_estimate=pl.CostEstimate(
            flops=12_000_000_000, bytes_accessed=10 * MIB, transcendentals=0
        ),
        name="pre",
    )(streams, branch)


def _owner(s, permuted):
    return jnp.bitwise_xor(lax.axis_index("dp"), s) if permuted else s


def raw_kernel(permuted, *refs):
    w_refs, (sde_ref, out_ref, wide_ref, lhs_ref) = refs[:-4], refs[-4:]
    count = w_refs[0].shape[0]
    pad = wide_ref.shape[1]
    blocks = sde_ref.shape[0]
    wide_ref[...] = jnp.zeros_like(wide_ref)
    for s in range(blocks):
        owner = _owner(s, permuted)
        for i in range(4):
            wide_ref[i, 0:count, :] = w_refs[s][:, i, :]
            hi, lo = _split(wide_ref[i])
            lhs_ref[owner, i, 0:pad, :] = hi
            lhs_ref[owner, i, pad : 2 * pad, :] = lo
    total = None
    for s in range(blocks):
        for i in range(4):
            part = _nt(lhs_ref[s, i], sde_ref[s, i])
            total = part if total is None else total + part
    rows = out_ref.shape[0]
    _store_by_column(out_ref, total[0:rows] + total[pad : pad + rows], 4)


def raw(weights, sde, permuted):
    blocks, _, tokens, _ = sde.shape
    return pl.pallas_call(
        functools.partial(raw_kernel, permuted),
        out_shape=jax.ShapeDtypeStruct((24, tokens), F32),
        in_specs=[VMEM] * (len(weights) + 1),
        out_specs=VMEM,
        scratch_shapes=[
            pltpu.VMEM((4, 32, FB), F32),
            pltpu.VMEM((blocks, 4, 64, FB), BF16),
        ],
        compiler_params=pltpu.CompilerParams(vmem_limit_bytes=12 * MIB),
        cost_estimate=pl.CostEstimate(
            flops=2_000_000_000, bytes_accessed=5 * MIB, transcendentals=0
        ),
        name="raw",
    )(*weights, sde)


def next_kernel(permuted, *refs):
    w_refs, (sde_ref, b_ref, out_ref, wide_ref, lhs_ref) = refs[:-5], refs[-5:]
    count = w_refs[0].shape[0]
    blocks = sde_ref.shape[0]
    rows = 4 * count
    for s in range(blocks):
        owner = _owner(s, permuted)
        for j in range(4):
            wide_ref[j * count : (j + 1) * count, :] = w_refs[s][:, j, :]
        hi, lo = _split(wide_ref[...])
        lhs_ref[owner, 0:rows, :] = hi
        lhs_ref[owner, rows : 2 * rows, :] = lo
    for i in range(5):
        total = None
        for s in range(blocks):
            right = sde_ref[s, i] if i < 4 else b_ref[:, s * FB : (s + 1) * FB]
            part = _nt(lhs_ref[s], right)
            total = part if total is None else total + part
        out_ref[i] = total[0:rows] + total[rows : 2 * rows]


def project_next(weights, sde, branch, permuted):
    blocks, _, tokens, _ = sde.shape
    rows = 4 * weights[0].shape[0]
    return pl.pallas_call(
        functools.partial(next_kernel, permuted),
        out_shape=jax.ShapeDtypeStruct((5, rows, tokens), F32),
        in_specs=[VMEM] * (len(weights) + 2),
        out_specs=VMEM,
        scratch_shapes=[
            pltpu.VMEM((rows, FB), F32),
            pltpu.VMEM((blocks, 2 * rows, FB), BF16),
        ],
        compiler_params=pltpu.CompilerParams(vmem_limit_bytes=14 * MIB),
        cost_estimate=pl.CostEstimate(
            flops=3_000_000_000, bytes_accessed=6 * MIB, transcendentals=0
        ),
        name="project_next",
    )(*weights, sde, branch)


def _balance(columns):
    for _ in range(BALANCE_ROUNDS):
        inverse = 1.0 / (columns[0] + columns[1] + columns[2] + columns[3])
        columns = [c * inverse for c in columns]
        columns = [c * (1.0 / jnp.sum(c, axis=0, keepdims=True)) for c in columns]
    return columns


def _sum4(refs, at):
    return (refs[0][at] + refs[1][at]) + (refs[2][at] + refs[3][at])


def first_kernel(features, *refs):
    r_refs, g_refs = refs[0:4], refs[4:8]
    bias_ref, scale_ref, pq_ref, coef_ref, next_ref, gram_ref = refs[8:]
    everything = (slice(None), slice(None))
    gram = _sum4(g_refs, everything)
    gram_ref[...] = gram
    squares = gram[0:1] + gram[4:5] + gram[7:8] + gram[9:10]
    inverse = 1.0 / jnp.sqrt(squares / features + EPS)
    raw_post = _sum4(r_refs, (slice(0, 4), slice(None)))
    post = 2.0 * jax.nn.sigmoid(scale_ref[0] * (raw_post * inverse) + bias_ref[0:4, :])
    columns = []
    for i in range(4):
        at = (slice(4 + 4 * i, 8 + 4 * i), slice(None))
        score = _sum4(r_refs, at) * inverse
        columns.append(jnp.exp(scale_ref[1] * score + bias_ref[at]))
    columns = _balance(columns)
    count = next_ref.shape[0]
    total = None
    for i in range(5):
        source = columns[i] if i < 4 else post
        coef_ref[4 * i : 4 * i + 4, :] = source
        for j in range(4):
            part = source[j : j + 1] * pq_ref[i, j * count : (j + 1) * count, :]
            total = part if total is None else total + part
    coef_ref[20:24, :] = jnp.zeros_like(coef_ref[20:24, :])
    _store_by_column(next_ref, total, 8)


def first(raws, grams, bias, scale, pq, features):
    tokens = pq.shape[2]
    return pl.pallas_call(
        functools.partial(first_kernel, features),
        out_shape=(
            jax.ShapeDtypeStruct((24, tokens), F32),
            jax.ShapeDtypeStruct((pq.shape[1] // 4, tokens), F32),
            jax.ShapeDtypeStruct((16, tokens), F32),
        ),
        in_specs=[VMEM] * 9 + [SMEM, VMEM],
        out_specs=(VMEM, VMEM, VMEM),
        compiler_params=pltpu.CompilerParams(vmem_limit_bytes=8 * MIB),
        cost_estimate=pl.CostEstimate(
            flops=1_000_000_000, bytes_accessed=MIB, transcendentals=20000
        ),
        name="first",
    )(*raws, *grams, bias, scale, pq)


def mix_kernel(coef_ref, sil_ref, b_ref, out_hbm, stage_ref, sems):
    tiles, tokens = sil_ref.shape[0], sil_ref.shape[1]
    rows = 4 * GT
    r32, m32 = _iota((rows, 32), 0), _iota((rows, 32), 1)
    keep = ((m32 % 4) == (r32 % 4)) & (m32 < 20)
    m_s, q_s = _iota((32, rows), 0), _iota((32, rows), 1)
    pick_stream = jnp.where((m_s // 4) == (q_s % 4), 1.0, 0.0).astype(BF16)
    m_b, q_b = _iota((32, GT), 0), _iota((32, GT), 1)
    pick_branch = jnp.where((m_b // 4) == 4, 1.0, 0.0).astype(BF16)
    same_stream = (_iota((rows, rows), 0) // 4) == (_iota((rows, rows), 1) // 4)
    same_branch = (_iota((rows, GT), 0) // 4) == _iota((rows, GT), 1)
    zero8 = jnp.zeros((8, tokens), F32)
    coef = jnp.concatenate([coef_ref[...], zero8], axis=0)
    parts = _split(coef)
    streams_of, branch_of = [], []
    for g in range(tokens // GT):
        half = g * GT // 128
        expand = jnp.where(
            _iota((rows, 128), 1) == (g * GT) % 128 + _iota((rows, 128), 0) // 4, 1.0, 0.0
        ).astype(BF16)
        for part in parts:
            held = _nt(expand, part[:, half * 128 : (half + 1) * 128])
            held = jnp.where(keep, held, 0.0).astype(BF16)
            wide = jnp.dot(held, pick_stream, preferred_element_type=F32)
            streams_of.append(jnp.where(same_stream, wide, 0.0).astype(BF16))
            wide = jnp.dot(held, pick_branch, preferred_element_type=F32)
            branch_of.append(jnp.where(same_branch, wide, 0.0).astype(BF16))

    def copy(c):
        return pltpu.make_async_copy(
            stage_ref.at[c],
            out_hbm.at[:, :, pl.ds(pl.multiple_of(c * 128, 128), 128)],
            sems.at[c],
        )

    def body(k, _):
        left = sil_ref.at[2 * k].reshape(4 * tokens, 128)
        right = sil_ref.at[2 * k + 1].reshape(4 * tokens, 128)
        out_left = stage_ref.at[2 * k].reshape(4 * tokens, 128)
        out_right = stage_ref.at[2 * k + 1].reshape(4 * tokens, 128)
        lanes = pl.ds(pl.multiple_of(k * FB, FB), FB)
        for g in range(tokens // GT):
            own = pl.ds(g * rows, rows)
            x = jnp.concatenate([left[own, :], right[own, :]], axis=1)
            b = b_ref[pl.ds(g * GT, GT), lanes]
            y = jnp.dot(streams_of[2 * g], x, preferred_element_type=F32)
            y += jnp.dot(streams_of[2 * g + 1], x, preferred_element_type=F32)
            y += jnp.dot(branch_of[2 * g], b, preferred_element_type=F32)
            y += jnp.dot(branch_of[2 * g + 1], b, preferred_element_type=F32)
            y = y.astype(BF16)
            out_left[own, :] = y[:, :128]
            out_right[own, :] = y[:, 128:]
        copy(2 * k).start()
        copy(2 * k + 1).start()
        return 0

    lax.fori_loop(0, tiles // 2, body, 0)
    for c in range(tiles):
        copy(c).wait()


def mix(coef, sil, branch):
    tiles, tokens = sil.shape[0], sil.shape[1]
    return pl.pallas_call(
        mix_kernel,
        out_shape=jax.ShapeDtypeStruct((tokens, 4, tiles * 128), BF16),
        in_specs=[VMEM, VMEM, VMEM],
        out_specs=HBM,
        scratch_shapes=[
            pltpu.VMEM((tiles, tokens, 4, 128), BF16),
            pltpu.SemaphoreType.DMA((tiles,)),
        ],
        compiler_params=pltpu.CompilerParams(vmem_limit_bytes=16 * MIB),
        cost_estimate=pl.CostEstimate(
            flops=5_000_000_000, bytes_accessed=8 * MIB, transcendentals=0
        ),
        name="mix",
    )(coef, sil, branch)


def second_kernel(features, *refs):
    r_refs = refs[0:4]
    coef_ref, gram_ref, bias_ref, scale_ref, sde_ref, b_ref, gain_ref = refs[4:11]
    out_ref, mix_ref, column_ref = refs[11:]
    tokens, width = b_ref.shape
    gram = gram_ref[...]
    columns = [coef_ref[4 * i : 4 * i + 4, :] for i in range(5)]

    def quadratic(terms):
        total = None
        for p, (i, j) in enumerate(PAIRS):
            part = terms[i] * terms[j] * gram[p : p + 1]
            part = part if i == j else 2.0 * part
            total = part if total is None else total + part
        for i in range(4):
            total = total + 2.0 * (terms[i] * terms[4]) * gram[10 + i : 11 + i]
        return total + terms[4] * terms[4] * gram[14:15]

    squares = jnp.maximum(jnp.sum(quadratic(columns), axis=0, keepdims=True), 0.0)
    inverse = 1.0 / jnp.sqrt(squares / features + EPS)
    everything = slice(None)
    pre_raw = _sum4(r_refs, (slice(0, 4), everything)) * inverse
    pre_next = jax.nn.sigmoid(scale_ref[2] * pre_raw + bias_ref[20:24, :])
    post_raw = _sum4(r_refs, (slice(4, 8), everything)) * inverse
    mix_ref[0:4, :] = 2.0 * jax.nn.sigmoid(scale_ref[3] * post_raw + bias_ref[24:28, :])
    following = []
    for i in range(4):
        score = _sum4(r_refs, (slice(8 + 4 * i, 12 + 4 * i), everything)) * inverse
        bias = bias_ref[28 + 4 * i : 32 + 4 * i, :]
        following.append(jnp.exp(scale_ref[4] * score + bias))
    following = _balance(following)
    for i in range(4):
        for j in range(4):
            mix_ref[4 + 4 * j + i : 5 + 4 * j + i, :] = following[i][j : j + 1]

    joint = [jnp.sum(pre_next * c, axis=0, keepdims=True) for c in columns]
    united = jnp.maximum(quadratic(joint), 0.0)
    root = 1.0 / jnp.sqrt(united / (features // 4) + EPS)
    stacked = jnp.concatenate([j * root for j in joint] + [jnp.zeros((3, tokens), F32)], axis=0)
    column_ref[:, 0:8] = stacked.T
    blocks = sde_ref.shape[0]

    def body(c, _):
        at = pl.ds(pl.multiple_of(c * 16, 16), 16)
        weights = [column_ref[at, i : i + 1] for i in range(5)]
        for k in range(blocks):
            lanes = pl.ds(k * FB, FB)
            total = weights[4] * b_ref[at, lanes].astype(F32)
            for i in range(4):
                total = total + weights[i] * sde_ref[k, i, at, :].astype(F32)
            out_ref[at, lanes] = (total * gain_ref[:, lanes]).astype(BF16)
        return 0

    lax.fori_loop(0, tokens // 16, body, 0)


def second(raws, coef, gram, bias, scale, sde, branch, gain, features):
    tokens, width = branch.shape
    return pl.pallas_call(
        functools.partial(second_kernel, features),
        out_shape=(
            jax.ShapeDtypeStruct((tokens, width), BF16),
            jax.ShapeDtypeStruct((20, tokens), F32),
        ),
        in_specs=[VMEM] * 7 + [SMEM] + [VMEM] * 3,
        out_specs=(VMEM, VMEM),
        scratch_shapes=[pltpu.VMEM((tokens, 128), F32)],
        compiler_params=pltpu.CompilerParams(vmem_limit_bytes=14 * MIB),
        cost_estimate=pl.CostEstimate(
            flops=3_000_000_000, bytes_accessed=6 * MIB, transcendentals=20000
        ),
        name="second",
    )(*raws, coef, gram, bias, scale, sde, branch, gain)


def _swap(x, axis, count, s):
    return lax.ppermute(x, axis, [(i, i ^ s) for i in range(count)])


def gather_blocks(weight, count, width):
    if weight.shape[2] == FB and count & (count - 1) == 0 and count * FB == width:
        even = {0: weight}
        for s in reversed(range(2, count, 2)):
            even[s] = _swap(weight, "dp", count, s)
        blocks = [None] * count
        for s in range(0, count, 2):
            blocks[s] = even[s]
            blocks[s + 1] = _swap(even[s], "dp", count, 1)
        return blocks, True
    whole = lax.all_gather(weight, "dp", axis=2, tiled=True)
    return [whole[:, :, k * FB : (k + 1) * FB] for k in range(width // FB)], False


def everyone(x, count):
    return [x] + [_swap(x, "mp", count, s) for s in range(1, count)]


def solution(mesh):
    n_dp, n_mp = mesh.shape["dp"], mesh.shape["mp"]

    def local(streams, branch, merge_weight, next_weight, blend_bias, blend_scale, norm_gain):
        tokens, count, width = streams.shape
        features = count * width * n_mp
        merge_blocks, permuted = gather_blocks(merge_weight, n_dp, width)
        next_blocks, _ = gather_blocks(next_weight, n_dp, width)
        by_column = [blend_bias[:4], blend_bias[4:20].reshape(4, 4).T.reshape(16)]
        by_column += [blend_bias[20:28], blend_bias[28:].reshape(4, 4).T.reshape(16)]
        bias = jnp.concatenate(by_column + [jnp.zeros((4,), F32)])
        bias = jnp.broadcast_to(bias[:, None], (48, tokens))
        gain = norm_gain[None, :]
        sil, sde, gram = pre(streams, branch)
        grams = everyone(gram, n_mp)
        raws = everyone(raw(merge_blocks, sde, permuted), n_mp)
        pq = project_next(next_blocks, sde, branch, permuted)
        coef, next_raw, gram_sum = first(raws, grams, bias, blend_scale, pq, features)
        next_raws = everyone(next_raw, n_mp)
        streams_out = mix(coef, sil, branch)
        branch_in, next_mix = second(
            next_raws, coef, gram_sum, bias, blend_scale, sde, branch, gain, features
        )
        return streams_out, branch_in, next_mix.T

    placed = (
        P("dp", None, "mp"),
        P("dp", "mp"),
        P(None, None, ("mp", "dp")),
        P(None, None, ("mp", "dp")),
        P(),
        P(),
        P("mp"),
    )
    return jax.shard_map(
        local,
        mesh=mesh,
        in_specs=placed,
        out_specs=(P("dp", None, "mp"), P("dp", "mp"), P("dp", None)),
        check_vma=False,
    )
```

```python
import functools

import jax
import jax.numpy as jnp
from jax import lax
from jax.experimental import pallas as pl
from jax.experimental.pallas import tpu as pltpu
from jax.sharding import PartitionSpec as P


BALANCE_ROUNDS = 6
EPS = 1e-06
FB = 256
GT = 64
MT = 32
F32 = jnp.float32
BF16 = jnp.bfloat16
MIB = 2**20

VMEM = pl.BlockSpec(memory_space=pltpu.VMEM)
SMEM = pl.BlockSpec(memory_space=pltpu.SMEM)
HBM = pl.BlockSpec(memory_space=pltpu.HBM)

PAIRS = [(i, j) for i in range(4) for j in range(i, 4)]


def _nt(a, b, precision=None):
    return lax.dot_general(
        a, b, (((1,), (1,)), ((), ())), precision=precision, preferred_element_type=F32
    )


def _split(x):
    hi = x.astype(BF16)
    return hi, (x - hi.astype(F32)).astype(BF16)


def _iota(shape, dim):
    return lax.broadcasted_iota(jnp.int32, shape, dim)


def _store_by_column(ref, rows, start):
    ref[0:start, :] = rows[0:start]
    for j in range(4):
        for i in range(4):
            source = start + 4 * j + i
            ref[start + 4 * i + j : start + 4 * i + j + 1, :] = rows[source : source + 1]
    if rows.shape[0] > start + 16:
        ref[start + 16 : rows.shape[0], :] = rows[start + 16 :]


def deal_kernel(s_hbm, sil_ref, sde_ref, sems):
    tokens, _, width = s_hbm.shape
    rows = 4 * tokens

    def copy(c):
        return pltpu.make_async_copy(
            s_hbm.at[:, :, pl.ds(pl.multiple_of(c * 128, 128), 128)], sil_ref.at[c], sems.at[c]
        )

    for c in range(width // 128):
        copy(c).start()
    r, q = _iota((4 * GT, 4 * GT), 0), _iota((4 * GT, 4 * GT), 1)
    perm = jnp.where(q == 4 * (r % GT) + r // GT, 1.0, 0.0).astype(BF16)

    def body(k, _):
        copy(2 * k).wait()
        copy(2 * k + 1).wait()
        left = sil_ref.at[2 * k].reshape(rows, 128)
        right = sil_ref.at[2 * k + 1].reshape(rows, 128)
        for g in range(tokens // GT):
            own = pl.ds(g * 4 * GT, 4 * GT)
            x = jnp.concatenate([left[own, :], right[own, :]], axis=1)
            y = jnp.dot(perm, x, preferred_element_type=F32)
            for i in range(4):
                sde_ref[k, i, pl.ds(g * GT, GT), :] = y[i * GT : (i + 1) * GT].astype(BF16)
        return 0

    lax.fori_loop(0, width // FB, body, 0)


def deal(streams):
    tokens, _, width = streams.shape
    return pl.pallas_call(
        deal_kernel,
        out_shape=(
            jax.ShapeDtypeStruct((width // 128, tokens, 4, 128), BF16),
            jax.ShapeDtypeStruct((width // FB, 4, tokens, FB), BF16),
        ),
        in_specs=[HBM],
        out_specs=(VMEM, VMEM),
        scratch_shapes=[pltpu.SemaphoreType.DMA((width // 128,))],
        compiler_params=pltpu.CompilerParams(vmem_limit_bytes=14 * MIB),
        cost_estimate=pl.CostEstimate(
            flops=4_000_000_000, bytes_accessed=10 * MIB, transcendentals=0
        ),
        name="deal",
    )(pltpu.with_memory_space_constraint(streams, pltpu.HBM))


def grams_kernel(sde_ref, b_ref, g_ref, column_ref):
    blocks, _, tokens, _ = sde_ref.shape

    def chunk(c, _):
        at = pl.ds(pl.multiple_of(c * 16, 16), 16)
        sums = [None] * 15
        for k in range(blocks):
            for h in range(FB // 128):
                lanes = slice(h * 128, (h + 1) * 128)
                wide = [sde_ref[k, i, at, lanes].astype(F32) for i in range(4)]
                wide.append(b_ref[at, k * FB + h * 128 : k * FB + (h + 1) * 128].astype(F32))
                products = [wide[i] * wide[j] for i, j in PAIRS]
                products += [wide[i] * wide[4] for i in range(5)]
                sums = [p if s is None else s + p for s, p in zip(sums, products)]
        lane = _iota((16, 128), 1)
        column = jnp.zeros((16, 128), F32)
        for p in range(15):
            column = jnp.where(lane == p, jnp.sum(sums[p], axis=1, keepdims=True), column)
        column_ref[at, :] = column
        return 0

    lax.fori_loop(0, tokens // 16, chunk, 0)
    g_ref[...] = column_ref[...].T[0:16]


def grams_of(sde, branch):
    tokens = sde.shape[2]
    return pl.pallas_call(
        grams_kernel,
        out_shape=jax.ShapeDtypeStruct((16, tokens), F32),
        in_specs=[VMEM, VMEM],
        out_specs=VMEM,
        scratch_shapes=[pltpu.VMEM((tokens, 128), F32)],
        compiler_params=pltpu.CompilerParams(vmem_limit_bytes=8 * MIB),
        cost_estimate=pl.CostEstimate(
            flops=3_000_000_000, bytes_accessed=5 * MIB, transcendentals=0
        ),
        name="grams",
    )(sde, branch)


def _owner(s, permuted):
    return jnp.bitwise_xor(lax.axis_index("dp"), s) if permuted else s


def raw_kernel(permuted, *refs):
    w_refs, (sde_ref, g_ref, out_ref, wide_ref, lhs_ref) = refs[:-5], refs[-5:]
    count = w_refs[0].shape[0]
    pad = wide_ref.shape[1]
    blocks = sde_ref.shape[0]
    wide_ref[...] = jnp.zeros_like(wide_ref)
    for s in range(blocks):
        owner = _owner(s, permuted)
        for i in range(4):
            wide_ref[i, 0:count, :] = w_refs[s][:, i, :]
            hi, lo = _split(wide_ref[i])
            lhs_ref[owner, i, 0:pad, :] = hi
            lhs_ref[owner, i, pad : 2 * pad, :] = lo
    total = None
    for s in range(blocks):
        for i in range(4):
            part = _nt(lhs_ref[s, i], sde_ref[s, i])
            total = part if total is None else total + part
    _store_by_column(out_ref, total[0:24] + total[pad : pad + 24], 4)
    out_ref[24:40, :] = g_ref[...]


def raw(weights, sde, gram, permuted):
    blocks, _, tokens, _ = sde.shape
    return pl.pallas_call(
        functools.partial(raw_kernel, permuted),
        out_shape=jax.ShapeDtypeStruct((40, tokens), F32),
        in_specs=[VMEM] * (len(weights) + 2),
        out_specs=VMEM,
        scratch_shapes=[
            pltpu.VMEM((4, 32, FB), F32),
            pltpu.VMEM((blocks, 4, 64, FB), BF16),
        ],
        compiler_params=pltpu.CompilerParams(vmem_limit_bytes=12 * MIB),
        cost_estimate=pl.CostEstimate(
            flops=2_000_000_000, bytes_accessed=5 * MIB, transcendentals=0
        ),
        name="raw",
    )(*weights, sde, gram)


def next_kernel(permuted, *refs):
    w_refs, (sde_ref, b_ref, coef_ref, out_ref, wide_ref, lhs_ref) = refs[:-6], refs[-6:]
    count = w_refs[0].shape[0]
    blocks = sde_ref.shape[0]
    rows = 4 * count
    for s in range(blocks):
        owner = _owner(s, permuted)
        for j in range(4):
            wide_ref[j * count : (j + 1) * count, :] = w_refs[s][:, j, :]
        hi, lo = _split(wide_ref[...])
        lhs_ref[owner, 0:rows, :] = hi
        lhs_ref[owner, rows : 2 * rows, :] = lo
    mixed = None
    for i in range(5):
        total = None
        for s in range(blocks):
            right = sde_ref[s, i] if i < 4 else b_ref[:, s * FB : (s + 1) * FB]
            part = _nt(lhs_ref[s], right)
            total = part if total is None else total + part
        total = total[0:rows] + total[rows : 2 * rows]
        for j in range(4):
            part = coef_ref[4 * i + j : 4 * i + j + 1, :] * total[j * count : (j + 1) * count]
            mixed = part if mixed is None else mixed + part
    _store_by_column(out_ref, mixed, 8)


def project_next(weights, sde, branch, coef, permuted):
    blocks, _, tokens, _ = sde.shape
    rows = 4 * weights[0].shape[0]
    return pl.pallas_call(
        functools.partial(next_kernel, permuted),
        out_shape=jax.ShapeDtypeStruct((rows // 4, tokens), F32),
        in_specs=[VMEM] * (len(weights) + 3),
        out_specs=VMEM,
        scratch_shapes=[
            pltpu.VMEM((rows, FB), F32),
            pltpu.VMEM((blocks, 2 * rows, FB), BF16),
        ],
        compiler_params=pltpu.CompilerParams(vmem_limit_bytes=14 * MIB),
        cost_estimate=pl.CostEstimate(
            flops=3_000_000_000, bytes_accessed=6 * MIB, transcendentals=0
        ),
        name="project_next",
    )(*weights, sde, branch, coef)


def _balance(columns):
    for _ in range(BALANCE_ROUNDS):
        inverse = 1.0 / (columns[0] + columns[1] + columns[2] + columns[3])
        columns = [c * inverse for c in columns]
        columns = [c * (1.0 / jnp.sum(c, axis=0, keepdims=True)) for c in columns]
    return columns


def _sum4(refs, at):
    return (refs[0][at] + refs[1][at]) + (refs[2][at] + refs[3][at])


def _bias(bias_ref, start, step):
    row = _iota((4, 128), 0)
    column = jnp.full((4, 128), bias_ref[start], F32)
    for j in range(1, 4):
        column = jnp.where(row == j, bias_ref[start + j * step], column)
    return column


def _scored(raw_rows, inverse, scale, bias):
    score = scale * (raw_rows * inverse)
    return score + jnp.concatenate([bias] * (score.shape[1] // 128), axis=1)


def first_kernel(features, *refs):
    r_refs = refs[0:4]
    bias_ref, scale_ref, coef_ref, gram_ref = refs[4:]
    gram = _sum4(r_refs, (slice(24, 40), slice(None)))
    gram_ref[...] = gram
    squares = gram[0:1] + gram[4:5] + gram[7:8] + gram[9:10]
    inverse = 1.0 / jnp.sqrt(squares / features + EPS)
    raw_post = _sum4(r_refs, (slice(0, 4), slice(None)))
    score = _scored(raw_post, inverse, scale_ref[0], _bias(bias_ref, 0, 1))
    coef_ref[16:20, :] = 2.0 * jax.nn.sigmoid(score)
    columns = []
    for i in range(4):
        raw_rows = _sum4(r_refs, (slice(4 + 4 * i, 8 + 4 * i), slice(None)))
        score = _scored(raw_rows, inverse, scale_ref[1], _bias(bias_ref, 4 + i, 4))
        columns.append(jnp.exp(score))
    columns = _balance(columns)
    for i in range(4):
        coef_ref[4 * i : 4 * i + 4, :] = columns[i]
    coef_ref[20:24, :] = jnp.zeros_like(coef_ref[20:24, :])


def first(raws, bias, scale, features):
    tokens = raws[0].shape[1]
    return pl.pallas_call(
        functools.partial(first_kernel, features),
        out_shape=(
            jax.ShapeDtypeStruct((24, tokens), F32),
            jax.ShapeDtypeStruct((16, tokens), F32),
        ),
        in_specs=[VMEM] * 4 + [SMEM, SMEM],
        out_specs=(VMEM, VMEM),
        compiler_params=pltpu.CompilerParams(vmem_limit_bytes=4 * MIB),
        cost_estimate=pl.CostEstimate(
            flops=1_000_000_000, bytes_accessed=MIB, transcendentals=20000
        ),
        name="first",
    )(*raws, bias, scale)


def mix_kernel(coef_ref, sil_ref, b_ref, out_hbm, stage_ref, left_ref, sems):
    tiles, tokens = sil_ref.shape[0], sil_ref.shape[1]
    rows = 4 * MT
    wide = 2 * rows + 2 * MT
    m, q = _iota((64, wide), 0), _iota((64, wide), 1)
    of_branch = q >= 2 * rows
    low = jnp.where(of_branch, (q - 2 * rows) // MT, q // rows)
    source = jnp.where(of_branch, 4, q % 4)
    pick = jnp.where(m // 4 == low * 8 + source, 1.0, 0.0).astype(BF16)
    r, q = _iota((rows, wide), 0), _iota((rows, wide), 1)
    token = jnp.where(q >= 2 * rows, (q - 2 * rows) % MT, (q % rows) // 4)
    same = token == r // 4
    r, m = _iota((rows, 64), 0), _iota((rows, 64), 1)
    keep = (m % 4) == (r % 4)
    hi, lo = _split(jnp.concatenate([coef_ref[...], jnp.zeros((8, tokens), F32)], axis=0))
    coef = jnp.concatenate([hi, lo], axis=0)
    for g in range(tokens // MT):
        start = g * MT // 128 * 128
        lane, r = _iota((rows, 128), 1), _iota((rows, 128), 0)
        expand = jnp.where(lane == g * MT - start + r // 4, 1.0, 0.0).astype(BF16)
        held = _nt(expand, coef[:, start : start + 128])
        held = jnp.where(keep, held, 0.0).astype(BF16)
        spread = jnp.dot(held, pick, preferred_element_type=F32)
        left_ref[g] = jnp.where(same, spread, 0.0).astype(BF16)

    def copy(c):
        return pltpu.make_async_copy(
            stage_ref.at[c],
            out_hbm.at[:, :, pl.ds(pl.multiple_of(c * 128, 128), 128)],
            sems.at[c],
        )

    def body(k, _):
        ins = [sil_ref.at[2 * k + h].reshape(4 * tokens, 128) for h in range(2)]
        outs = [stage_ref.at[2 * k + h].reshape(4 * tokens, 128) for h in range(2)]
        lanes = pl.ds(pl.multiple_of(k * FB, FB), FB)
        for g in range(tokens // MT):
            own = pl.ds(g * rows, rows)
            x = jnp.concatenate([ins[0][own, :], ins[1][own, :]], axis=1)
            b = b_ref[pl.ds(g * MT, MT), lanes]
            y = jnp.dot(
                left_ref[g, :, 0 : 2 * rows],
                jnp.concatenate([x, x], axis=0),
                preferred_element_type=F32,
            )
            y += jnp.dot(
                left_ref[g, :, 2 * rows : wide],
                jnp.concatenate([b, b], axis=0),
                preferred_element_type=F32,
            )
            y = y.astype(BF16)
            outs[0][own, :] = y[:, :128]
            outs[1][own, :] = y[:, 128:]
        copy(2 * k).start()
        copy(2 * k + 1).start()
        return 0

    lax.fori_loop(0, tiles // 2, body, 0)
    for c in range(tiles):
        copy(c).wait()


def mix(coef, sil, branch):
    tiles, tokens = sil.shape[0], sil.shape[1]
    return pl.pallas_call(
        mix_kernel,
        out_shape=jax.ShapeDtypeStruct((tokens, 4, tiles * 128), BF16),
        in_specs=[VMEM, VMEM, VMEM],
        out_specs=HBM,
        scratch_shapes=[
            pltpu.VMEM((tiles, tokens, 4, 128), BF16),
            pltpu.VMEM((tokens // MT, 4 * MT, 10 * MT), BF16),
            pltpu.SemaphoreType.DMA((tiles,)),
        ],
        compiler_params=pltpu.CompilerParams(vmem_limit_bytes=14 * MIB),
        cost_estimate=pl.CostEstimate(
            flops=5_000_000_000, bytes_accessed=8 * MIB, transcendentals=0
        ),
        name="mix",
    )(coef, sil, branch)


def second_kernel(features, *refs):
    r_refs = refs[0:4]
    coef_ref, gram_ref, bias_ref, scale_ref, sde_ref, b_ref, gain_ref = refs[4:11]
    out_ref, mix_ref, column_ref = refs[11:]
    tokens, _ = b_ref.shape
    gram = gram_ref[...]
    columns = [coef_ref[4 * i : 4 * i + 4, :] for i in range(5)]

    def quadratic(terms):
        total = None
        for p, (i, j) in enumerate(PAIRS):
            part = terms[i] * terms[j] * gram[p : p + 1]
            part = part if i == j else 2.0 * part
            total = part if total is None else total + part
        for i in range(4):
            total = total + 2.0 * (terms[i] * terms[4]) * gram[10 + i : 11 + i]
        return total + terms[4] * terms[4] * gram[14:15]

    squares = jnp.maximum(jnp.sum(quadratic(columns), axis=0, keepdims=True), 0.0)
    inverse = 1.0 / jnp.sqrt(squares / features + EPS)
    everything = slice(None)
    pre_raw = _sum4(r_refs, (slice(0, 4), everything))
    score = _scored(pre_raw, inverse, scale_ref[2], _bias(bias_ref, 20, 1))
    pre_next = jax.nn.sigmoid(score)
    post_raw = _sum4(r_refs, (slice(4, 8), everything))
    score = _scored(post_raw, inverse, scale_ref[3], _bias(bias_ref, 24, 1))
    mix_ref[0:4, :] = 2.0 * jax.nn.sigmoid(score)
    following = []
    for i in range(4):
        raw_rows = _sum4(r_refs, (slice(8 + 4 * i, 12 + 4 * i), everything))
        score = _scored(raw_rows, inverse, scale_ref[4], _bias(bias_ref, 28 + i, 4))
        following.append(jnp.exp(score))
    following = _balance(following)
    for i in range(4):
        for j in range(4):
            mix_ref[4 + 4 * j + i : 5 + 4 * j + i, :] = following[i][j : j + 1]

    joint = [jnp.sum(pre_next * c, axis=0, keepdims=True) for c in columns]
    united = jnp.maximum(quadratic(joint), 0.0)
    root = 1.0 / jnp.sqrt(united / (features // 4) + EPS)
    stacked = jnp.concatenate([j * root for j in joint] + [jnp.zeros((3, tokens), F32)], axis=0)
    column_ref[:, 0:8] = stacked.T
    blocks = sde_ref.shape[0]

    def body(c, _):
        at = pl.ds(pl.multiple_of(c * 16, 16), 16)
        weights = [column_ref[at, i : i + 1] for i in range(5)]
        for k in range(blocks):
            lanes = pl.ds(k * FB, FB)
            total = weights[4] * b_ref[at, lanes].astype(F32)
            for i in range(4):
                total = total + weights[i] * sde_ref[k, i, at, :].astype(F32)
            out_ref[at, lanes] = (total * gain_ref[:, lanes]).astype(BF16)
        return 0

    lax.fori_loop(0, tokens // 16, body, 0)


def second(raws, coef, gram, bias, scale, sde, branch, gain, features):
    tokens, width = branch.shape
    return pl.pallas_call(
        functools.partial(second_kernel, features),
        out_shape=(
            jax.ShapeDtypeStruct((tokens, width), BF16),
            jax.ShapeDtypeStruct((20, tokens), F32),
        ),
        in_specs=[VMEM] * 6 + [SMEM] * 2 + [VMEM] * 3,
        out_specs=(VMEM, VMEM),
        scratch_shapes=[pltpu.VMEM((tokens, 128), F32)],
        compiler_params=pltpu.CompilerParams(vmem_limit_bytes=14 * MIB),
        cost_estimate=pl.CostEstimate(
            flops=3_000_000_000, bytes_accessed=6 * MIB, transcendentals=20000
        ),
        name="second",
    )(*raws, coef, gram, bias, scale, sde, branch, gain)


def _swap(x, axis, count, s):
    return lax.ppermute(x, axis, [(i, i ^ s) for i in range(count)])


def gather_blocks(weight, count, width):
    if weight.shape[2] == FB and count & (count - 1) == 0 and count * FB == width:
        even = {0: weight}
        for s in range(2, count, 2):
            even[s] = _swap(weight, "dp", count, s)
        blocks = [None] * count
        for s in range(0, count, 2):
            blocks[s] = even[s]
            blocks[s + 1] = _swap(even[s], "dp", count, 1)
        return blocks, True
    whole = lax.all_gather(weight, "dp", axis=2, tiled=True)
    return [whole[:, :, k * FB : (k + 1) * FB] for k in range(width // FB)], False


def everyone(x, count):
    return [x] + [_swap(x, "mp", count, s) for s in range(1, count)]


def solution(mesh):
    n_dp, n_mp = mesh.shape["dp"], mesh.shape["mp"]

    def local(streams, branch, merge_weight, next_weight, blend_bias, blend_scale, norm_gain):
        count, width = streams.shape[1:]
        features = count * width * n_mp
        merge_blocks, permuted = gather_blocks(merge_weight, n_dp, width)
        next_blocks, _ = gather_blocks(next_weight, n_dp, width)
        gain = norm_gain[None, :]
        sil, sde = deal(streams)
        gram = grams_of(sde, branch)
        raws = everyone(raw(merge_blocks, sde, gram, permuted), n_mp)
        coef, gram_sum = first(raws, blend_bias, blend_scale, features)
        streams_out = mix(coef, sil, branch)
        next_raw = project_next(next_blocks, sde, branch, coef, permuted)
        next_raws = everyone(next_raw, n_mp)
        branch_in, next_mix = second(
            next_raws, coef, gram_sum, blend_bias, blend_scale, sde, branch, gain, features
        )
        return streams_out, branch_in, next_mix.T

    placed = (
        P("dp", None, "mp"),
        P("dp", "mp"),
        P(None, None, ("mp", "dp")),
        P(None, None, ("mp", "dp")),
        P(),
        P(),
        P("mp"),
    )
    return jax.shard_map(
        local,
        mesh=mesh,
        in_specs=placed,
        out_specs=(P("dp", None, "mp"), P("dp", "mp"), P("dp", None)),
        check_vma=False,
    )
```

```python
import functools

import jax
import jax.numpy as jnp
from jax import lax
from jax.experimental import pallas as pl
from jax.experimental.pallas import tpu as pltpu
from jax.sharding import PartitionSpec as P


BALANCE_ROUNDS = 6
EPS = 1e-06
FB = 256
GT = 64
MT = 16
F32 = jnp.float32
BF16 = jnp.bfloat16
MIB = 2**20

VMEM = pl.BlockSpec(memory_space=pltpu.VMEM)
HBM = pl.BlockSpec(memory_space=pltpu.HBM)

PAIRS = [(i, j) for i in range(4) for j in range(i, 4)]


def _nt(a, b, precision=None):
    return lax.dot_general(
        a, b, (((1,), (1,)), ((), ())), precision=precision, preferred_element_type=F32
    )


def _split(x):
    hi = x.astype(BF16)
    return hi, (x - hi.astype(F32)).astype(BF16)


def _iota(shape, dim):
    return lax.broadcasted_iota(jnp.int32, shape, dim)


def _store_by_column(ref, rows, start):
    ref[0:start, :] = rows[0:start]
    for j in range(4):
        for i in range(4):
            source = start + 4 * j + i
            ref[start + 4 * i + j : start + 4 * i + j + 1, :] = rows[source : source + 1]
    if rows.shape[0] > start + 16:
        ref[start + 16 : rows.shape[0], :] = rows[start + 16 :]


def deal_kernel(s_hbm, sil_ref, sde_ref, q_ref, part_ref, sems):
    tokens, _, width = s_hbm.shape
    rows = 4 * GT
    flat = s_hbm.reshape(4 * tokens, width)

    def copy(c):
        return pltpu.make_async_copy(
            flat.at[:, pl.ds(pl.multiple_of(c * 128, 128), 128)], sil_ref.at[c], sems.at[c]
        )

    for c in range(width // 128):
        copy(c).start()
    r, q = _iota((rows, rows), 0), _iota((rows, rows), 1)
    perm = jnp.where(q == 4 * (r % GT) + r // GT, 1.0, 0.0).astype(BF16)
    part_ref[...] = jnp.zeros_like(part_ref)

    def body(k, _):
        copy(2 * k).wait()
        copy(2 * k + 1).wait()
        for g in range(tokens // GT):
            own, mine = pl.ds(g * rows, rows), pl.ds(g * GT, GT)
            x = jnp.concatenate([sil_ref[2 * k, own, :], sil_ref[2 * k + 1, own, :]], axis=1)
            y = jnp.dot(perm, x, preferred_element_type=F32)
            for i in range(4):
                sde_ref[k, i, mine, :] = y[i * GT : (i + 1) * GT].astype(BF16)
            y = y * y
            y = (y[0:GT] + y[GT : 2 * GT]) + (y[2 * GT : 3 * GT] + y[3 * GT :])
            part_ref[mine, :] += y[:, :128] + y[:, 128:]
        return 0

    lax.fori_loop(0, width // FB, body, 0)
    q_ref[...] = jnp.sum(part_ref[...].T.reshape(16, 8, tokens), axis=0)


def deal(streams):
    tokens, _, width = streams.shape
    tiles = width // 128
    return pl.pallas_call(
        deal_kernel,
        out_shape=(
            jax.ShapeDtypeStruct((tiles, 4 * tokens, 128), BF16),
            jax.ShapeDtypeStruct((width // FB, 4, tokens, FB), BF16),
            jax.ShapeDtypeStruct((8, tokens), F32),
        ),
        in_specs=[HBM],
        out_specs=(VMEM, VMEM, VMEM),
        scratch_shapes=[pltpu.VMEM((tokens, 128), F32), pltpu.SemaphoreType.DMA((tiles,))],
        compiler_params=pltpu.CompilerParams(vmem_limit_bytes=20 * MIB),
        cost_estimate=pl.CostEstimate(
            flops=6_000_000_000, bytes_accessed=10 * MIB, transcendentals=0
        ),
        name="deal",
    )(pltpu.with_memory_space_constraint(streams, pltpu.HBM))


def grams_kernel(sde_ref, b_ref, g_ref, column_ref):
    blocks, _, tokens, _ = sde_ref.shape

    def chunk(c, _):
        at = pl.ds(pl.multiple_of(c * 16, 16), 16)
        sums = [None] * 15
        for k in range(blocks):
            for h in range(FB // 128):
                lanes = slice(h * 128, (h + 1) * 128)
                wide = [sde_ref[k, i, at, lanes].astype(F32) for i in range(4)]
                wide.append(b_ref[at, k * FB + h * 128 : k * FB + (h + 1) * 128].astype(F32))
                products = [wide[i] * wide[j] for i, j in PAIRS]
                products += [wide[i] * wide[4] for i in range(5)]
                sums = [p if s is None else s + p for s, p in zip(sums, products)]
        lane = _iota((16, 128), 1)
        column = jnp.zeros((16, 128), F32)
        for p in range(15):
            column = jnp.where(lane == p, jnp.sum(sums[p], axis=1, keepdims=True), column)
        column_ref[at, :] = column
        return 0

    lax.fori_loop(0, tokens // 16, chunk, 0)
    g_ref[...] = column_ref[...].T[0:16]


def grams_of(sde, branch):
    tokens = sde.shape[2]
    return pl.pallas_call(
        grams_kernel,
        out_shape=jax.ShapeDtypeStruct((16, tokens), F32),
        in_specs=[VMEM, VMEM],
        out_specs=VMEM,
        scratch_shapes=[pltpu.VMEM((tokens, 128), F32)],
        compiler_params=pltpu.CompilerParams(vmem_limit_bytes=8 * MIB),
        cost_estimate=pl.CostEstimate(
            flops=3_000_000_000, bytes_accessed=5 * MIB, transcendentals=0
        ),
        name="grams",
    )(sde, branch)


def _owner(s, permuted):
    return jnp.bitwise_xor(lax.axis_index("dp"), s) if permuted else s


def raw_kernel(permuted, *refs):
    w_refs, (sde_ref, q_ref, out_ref, wide_ref, lhs_ref) = refs[:-5], refs[-5:]
    count = w_refs[0].shape[0]
    pad = wide_ref.shape[1]
    blocks = sde_ref.shape[0]
    wide_ref[...] = jnp.zeros_like(wide_ref)
    for s in range(blocks):
        owner = _owner(s, permuted)
        for i in range(4):
            wide_ref[i, 0:count, :] = w_refs[s][:, i, :]
            hi, lo = _split(wide_ref[i])
            lhs_ref[owner, i, 0:pad, :] = hi
            lhs_ref[owner, i, pad : 2 * pad, :] = lo
    total = None
    for s in range(blocks):
        for i in range(4):
            part = _nt(lhs_ref[s, i], sde_ref[s, i])
            total = part if total is None else total + part
    _store_by_column(out_ref, total[0:20] + total[pad : pad + 20], 4)
    out_ref[20:21, :] = jnp.sum(q_ref[...], axis=0, keepdims=True)
    out_ref[21:24, :] = jnp.zeros((3, out_ref.shape[1]), F32)


def raw(weights, sde, squares, permuted):
    blocks, _, tokens, _ = sde.shape
    return pl.pallas_call(
        functools.partial(raw_kernel, permuted),
        out_shape=jax.ShapeDtypeStruct((24, tokens), F32),
        in_specs=[VMEM] * (len(weights) + 2),
        out_specs=VMEM,
        scratch_shapes=[
            pltpu.VMEM((4, 32, FB), F32),
            pltpu.VMEM((blocks, 4, 64, FB), BF16),
        ],
        compiler_params=pltpu.CompilerParams(vmem_limit_bytes=12 * MIB),
        cost_estimate=pl.CostEstimate(
            flops=2_000_000_000, bytes_accessed=5 * MIB, transcendentals=0
        ),
        name="raw",
    )(*weights, sde, squares)


def pair_kernel(*refs):
    w_refs, out_ref = refs[:-1], refs[-1]
    count = w_refs[0].shape[0]
    for s, w_ref in enumerate(w_refs):
        for j in range(4):
            out_ref[s, j * count : (j + 1) * count, :] = w_ref[:, j, :]


def pair(*weights):
    count = weights[0].shape[0]
    return pl.pallas_call(
        pair_kernel,
        out_shape=jax.ShapeDtypeStruct((len(weights), 4 * count, FB), F32),
        in_specs=[VMEM] * len(weights),
        out_specs=VMEM,
        compiler_params=pltpu.CompilerParams(vmem_limit_bytes=4 * MIB),
        cost_estimate=pl.CostEstimate(flops=100_000_000, bytes_accessed=MIB, transcendentals=0),
        name="pair",
    )(*weights)


def next_kernel(order, permuted, *refs):
    w_refs, (sde_ref, b_ref, coef_ref, g_ref, out_ref, lhs_ref) = refs[:-6], refs[-6:]
    rows = w_refs[0].shape[1]
    count = rows // 4
    blocks = sde_ref.shape[0]
    places = [(w_ref, n) for w_ref in w_refs for n in range(w_ref.shape[0])]
    for s, (w_ref, n) in zip(order, places):
        owner = _owner(s, permuted)
        hi, lo = _split(w_ref[n])
        lhs_ref[owner, 0:rows, :] = hi
        lhs_ref[owner, rows : 2 * rows, :] = lo
    mixed = None
    for i in range(5):
        total = None
        for s in range(blocks):
            right = sde_ref[s, i] if i < 4 else b_ref[:, s * FB : (s + 1) * FB]
            part = _nt(lhs_ref[s], right)
            total = part if total is None else total + part
        total = total[0:rows] + total[rows : 2 * rows]
        for j in range(4):
            part = coef_ref[4 * i + j : 4 * i + j + 1, :] * total[j * count : (j + 1) * count]
            mixed = part if mixed is None else mixed + part
    _store_by_column(out_ref, mixed, 8)
    out_ref[count:, :] = g_ref[...]


def project_next(weights, order, sde, branch, coef, gram, permuted):
    blocks, _, tokens, _ = sde.shape
    rows = weights[0].shape[1]
    return pl.pallas_call(
        functools.partial(next_kernel, order, permuted),
        out_shape=jax.ShapeDtypeStruct((rows // 4 + gram.shape[0], tokens), F32),
        in_specs=[VMEM] * (len(weights) + 4),
        out_specs=VMEM,
        scratch_shapes=[pltpu.VMEM((blocks, 2 * rows, FB), BF16)],
        compiler_params=pltpu.CompilerParams(vmem_limit_bytes=14 * MIB),
        cost_estimate=pl.CostEstimate(
            flops=3_000_000_000, bytes_accessed=6 * MIB, transcendentals=0
        ),
        name="project_next",
    )(*weights, sde, branch, coef, gram)


def _balance(columns):
    for _ in range(BALANCE_ROUNDS):
        inverse = 1.0 / (columns[0] + columns[1] + columns[2] + columns[3])
        columns = [c * inverse for c in columns]
        columns = [c * (1.0 / jnp.sum(c, axis=0, keepdims=True)) for c in columns]
    return columns


def _sum4(refs, at):
    return (refs[0][at] + refs[1][at]) + (refs[2][at] + refs[3][at])


def _column(ref, start, step):
    wide = ref.shape[1]
    here = _iota((4, wide), 1) == start + step * _iota((4, wide), 0)
    return jnp.sum(jnp.where(here, jnp.broadcast_to(ref[...], (4, wide)), 0.0), axis=1, keepdims=True)


def _scored(raw_rows, inverse, scale, bias):
    return scale * (raw_rows * inverse) + bias


def first_kernel(features, *refs):
    r_refs = refs[0:4]
    bias_ref, scale_ref, coef_ref = refs[4:]
    squares = _sum4(r_refs, (slice(20, 21), slice(None)))
    inverse = 1.0 / jnp.sqrt(squares / features + EPS)
    raw_post = _sum4(r_refs, (slice(0, 4), slice(None)))
    score = _scored(raw_post, inverse, _column(scale_ref, 0, 0), _column(bias_ref, 0, 1))
    coef_ref[16:20, :] = 2.0 * jax.nn.sigmoid(score)
    columns = []
    for i in range(4):
        raw_rows = _sum4(r_refs, (slice(4 + 4 * i, 8 + 4 * i), slice(None)))
        score = _scored(raw_rows, inverse, _column(scale_ref, 1, 0), _column(bias_ref, 4 + i, 4))
        columns.append(jnp.exp(score))
    columns = _balance(columns)
    for i in range(4):
        coef_ref[4 * i : 4 * i + 4, :] = columns[i]
    coef_ref[20:24, :] = jnp.zeros_like(coef_ref[20:24, :])


def first(raws, bias, scale, features):
    tokens = raws[0].shape[1]
    return pl.pallas_call(
        functools.partial(first_kernel, features),
        out_shape=jax.ShapeDtypeStruct((24, tokens), F32),
        in_specs=[VMEM] * 6,
        out_specs=VMEM,
        compiler_params=pltpu.CompilerParams(vmem_limit_bytes=4 * MIB),
        cost_estimate=pl.CostEstimate(
            flops=1_000_000_000, bytes_accessed=MIB, transcendentals=20000
        ),
        name="first",
    )(*raws, bias, scale)


def weave_kernel(coef_ref, left_ref):
    tokens = coef_ref.shape[1]
    rows = 4 * MT
    wide = 2 * rows + 2 * MT
    m, q = _iota((64, wide), 0), _iota((64, wide), 1)
    of_branch = q >= 2 * rows
    low = jnp.where(of_branch, (q - 2 * rows) // MT, q // rows)
    source = jnp.where(of_branch, 4, q % 4)
    pick = jnp.where(m // 4 == low * 8 + source, 1.0, 0.0).astype(BF16)
    r, q = _iota((rows, wide), 0), _iota((rows, wide), 1)
    token = jnp.where(q >= 2 * rows, (q - 2 * rows) % MT, (q % rows) // 4)
    same = token == r // 4
    r, m = _iota((rows, 64), 0), _iota((rows, 64), 1)
    keep = (m % 4) == (r % 4)
    hi, lo = _split(jnp.concatenate([coef_ref[...], jnp.zeros((8, tokens), F32)], axis=0))
    coef = jnp.concatenate([hi, lo], axis=0)
    for g in range(tokens // MT):
        start = g * MT // 128 * 128
        lane, r = _iota((rows, 128), 1), _iota((rows, 128), 0)
        expand = jnp.where(lane == g * MT - start + r // 4, 1.0, 0.0).astype(BF16)
        held = _nt(expand, coef[:, start : start + 128])
        held = jnp.where(keep, held, 0.0).astype(BF16)
        spread = jnp.dot(held, pick, preferred_element_type=F32)
        left_ref[g] = jnp.where(same, spread, 0.0).astype(BF16)


def weave(coef):
    tokens = coef.shape[1]
    return pl.pallas_call(
        weave_kernel,
        out_shape=jax.ShapeDtypeStruct((tokens // MT, 4 * MT, 10 * MT), BF16),
        in_specs=[VMEM],
        out_specs=VMEM,
        compiler_params=pltpu.CompilerParams(vmem_limit_bytes=6 * MIB),
        cost_estimate=pl.CostEstimate(
            flops=1_000_000_000, bytes_accessed=MIB, transcendentals=0
        ),
        name="weave",
    )(coef)


def mix_kernel(left_ref, sil_ref, b_ref, out_hbm, stage_ref, sems):
    tiles, tokens = sil_ref.shape[0], sil_ref.shape[1] // 4
    rows = 4 * MT
    flat = out_hbm.reshape(4 * tokens, tiles * 128)

    def copy(c):
        return pltpu.make_async_copy(
            stage_ref.at[c], flat.at[:, pl.ds(pl.multiple_of(c * 128, 128), 128)], sems.at[c]
        )

    def body(k, _):
        lanes = pl.ds(pl.multiple_of(k * FB, FB), FB)
        for g in range(tokens // MT):
            own = pl.ds(g * rows, rows)
            x = jnp.concatenate([sil_ref[2 * k, own, :], sil_ref[2 * k + 1, own, :]], axis=1)
            b = b_ref[pl.ds(g * MT, MT), lanes]
            right = jnp.concatenate([x, x, b, b], axis=0)
            y = jnp.dot(left_ref[g], right, preferred_element_type=F32)
            y = y.astype(BF16)
            stage_ref[2 * k, own, :] = y[:, :128]
            stage_ref[2 * k + 1, own, :] = y[:, 128:]
        copy(2 * k).start()
        copy(2 * k + 1).start()
        return 0

    lax.fori_loop(0, tiles // 2, body, 0)
    for c in range(tiles):
        copy(c).wait()


def mix(left, sil, branch):
    tiles, tokens = sil.shape[0], sil.shape[1] // 4
    return pl.pallas_call(
        mix_kernel,
        out_shape=jax.ShapeDtypeStruct((tokens, 4, tiles * 128), BF16),
        in_specs=[VMEM, VMEM, VMEM],
        out_specs=HBM,
        scratch_shapes=[
            pltpu.VMEM((tiles, 4 * tokens, 128), BF16),
            pltpu.SemaphoreType.DMA((tiles,)),
        ],
        compiler_params=pltpu.CompilerParams(vmem_limit_bytes=14 * MIB),
        cost_estimate=pl.CostEstimate(
            flops=5_000_000_000, bytes_accessed=8 * MIB, transcendentals=0
        ),
        name="mix",
    )(left, sil, branch)


def second_kernel(features, *refs):
    r_refs = refs[0:4]
    coef_ref, bias_ref, scale_ref, sde_ref, b_ref, gain_ref = refs[4:10]
    out_hbm, mix_hbm, mix_ref, column_ref, out_ref, sems, mix_sem = refs[10:]
    tokens, _ = b_ref.shape
    gram = _sum4(r_refs, (slice(24, 40), slice(None)))
    columns = [coef_ref[4 * i : 4 * i + 4, :] for i in range(5)]

    def quadratic(terms):
        total = None
        for p, (i, j) in enumerate(PAIRS):
            part = terms[i] * terms[j] * gram[p : p + 1]
            part = part if i == j else 2.0 * part
            total = part if total is None else total + part
        for i in range(4):
            total = total + 2.0 * (terms[i] * terms[4]) * gram[10 + i : 11 + i]
        return total + terms[4] * terms[4] * gram[14:15]

    squares = jnp.maximum(jnp.sum(quadratic(columns), axis=0, keepdims=True), 0.0)
    inverse = 1.0 / jnp.sqrt(squares / features + EPS)
    everything = slice(None)
    pre_raw = _sum4(r_refs, (slice(0, 4), everything))
    score = _scored(pre_raw, inverse, _column(scale_ref, 2, 0), _column(bias_ref, 20, 1))
    pre_next = jax.nn.sigmoid(score)
    post_raw = _sum4(r_refs, (slice(4, 8), everything))
    score = _scored(post_raw, inverse, _column(scale_ref, 3, 0), _column(bias_ref, 24, 1))
    mix_ref[0:4, :] = 2.0 * jax.nn.sigmoid(score)
    following = []
    for i in range(4):
        raw_rows = _sum4(r_refs, (slice(8 + 4 * i, 12 + 4 * i), everything))
        score = _scored(raw_rows, inverse, _column(scale_ref, 4, 0), _column(bias_ref, 28 + i, 4))
        following.append(jnp.exp(score))
    following = _balance(following)
    for i in range(4):
        for j in range(4):
            mix_ref[4 + 4 * j + i : 5 + 4 * j + i, :] = following[i][j : j + 1]
    mix_copy = pltpu.make_async_copy(mix_ref, mix_hbm, mix_sem)
    mix_copy.start()

    joint = [jnp.sum(pre_next * c, axis=0, keepdims=True) for c in columns]
    united = jnp.maximum(quadratic(joint), 0.0)
    root = 1.0 / jnp.sqrt(united / (features // 4) + EPS)
    stacked = jnp.concatenate([j * root for j in joint] + [jnp.zeros((3, tokens), F32)], axis=0)
    column_ref[:, 0:8] = stacked.T
    blocks = sde_ref.shape[0]

    def copy(c):
        at = pl.ds(pl.multiple_of(c * 16, 16), 16)
        return pltpu.make_async_copy(out_ref.at[at], out_hbm.at[at], sems.at[c])

    def body(c, _):
        at = pl.ds(pl.multiple_of(c * 16, 16), 16)
        weights = [column_ref[at, i : i + 1] for i in range(5)]
        for k in range(blocks):
            lanes = pl.ds(k * FB, FB)
            total = weights[4] * b_ref[at, lanes].astype(F32)
            for i in range(4):
                total = total + weights[i] * sde_ref[k, i, at, :].astype(F32)
            out_ref[at, lanes] = (total * gain_ref[:, lanes]).astype(BF16)
        copy(c).start()
        return 0

    lax.fori_loop(0, tokens // 16, body, 0)
    for c in range(tokens // 16):
        copy(c).wait()
    mix_copy.wait()


def second(raws, coef, bias, scale, sde, branch, gain, features):
    tokens, width = branch.shape
    return pl.pallas_call(
        functools.partial(second_kernel, features),
        out_shape=(
            jax.ShapeDtypeStruct((tokens, width), BF16),
            jax.ShapeDtypeStruct((20, tokens), F32),
        ),
        in_specs=[VMEM] * 10,
        out_specs=(HBM, HBM),
        scratch_shapes=[
            pltpu.VMEM((20, tokens), F32),
            pltpu.VMEM((tokens, 128), F32),
            pltpu.VMEM((tokens, width), BF16),
            pltpu.SemaphoreType.DMA((tokens // 16,)),
            pltpu.SemaphoreType.DMA,
        ],
        compiler_params=pltpu.CompilerParams(vmem_limit_bytes=14 * MIB),
        cost_estimate=pl.CostEstimate(
            flops=3_000_000_000, bytes_accessed=6 * MIB, transcendentals=20000
        ),
        name="second",
    )(*raws, coef, bias, scale, sde, branch, gain)


def _swap(x, axis, count, s):
    return lax.ppermute(x, axis, [(i, i ^ s) for i in range(count)])


def by_block(weight, width):
    whole = lax.all_gather(weight, "dp", axis=2, tiled=True)
    return [whole[:, :, k * FB : (k + 1) * FB] for k in range(width // FB)]


def gather_merge(weight, count, width):
    if count != 8 or count * weight.shape[2] != width or weight.shape[2] != FB:
        return by_block(weight, width), False
    blocks = {0: weight}
    for s in (2, 4, 6):
        blocks[s] = _swap(weight, "dp", count, s)
    for s in (0, 2, 4, 6):
        blocks[s + 1] = _swap(blocks[s], "dp", count, 1)
    return [blocks[s] for s in range(count)], True


def gather_next(weight, count, width):
    if count != 8 or count * weight.shape[2] != width or weight.shape[2] != FB:
        return [pair(*by_block(weight, width))], tuple(range(width // FB))
    far = _swap(weight, "dp", count, 2)
    here = pair(weight, far)
    there = _swap(here, "dp", count, 4)
    near = _swap(here, "dp", count, 1)
    across = _swap(there, "dp", count, 1)
    return [here, near, there, across], (0, 2, 1, 3, 4, 6, 5, 7)


def everyone(x, count):
    return [x] + [_swap(x, "mp", count, s) for s in range(1, count)]


def solution(mesh):
    n_dp, n_mp = mesh.shape["dp"], mesh.shape["mp"]

    def local(streams, branch, merge_weight, next_weight, blend_bias, blend_scale, norm_gain):
        count, width = streams.shape[1:]
        features = count * width * n_mp
        merge_blocks, permuted = gather_merge(merge_weight, n_dp, width)
        next_blocks, order = gather_next(next_weight, n_dp, width)
        gain, bias, scale = norm_gain[None, :], blend_bias[None, :], blend_scale[None, :]
        sil, sde, squares = deal(streams)
        gram = grams_of(sde, branch)
        raws = everyone(raw(merge_blocks, sde, squares, permuted), n_mp)
        coef = first(raws, bias, scale, features)
        streams_out = mix(weave(coef), sil, branch)
        next_raw = project_next(next_blocks, order, sde, branch, coef, gram, permuted)
        next_raws = everyone(next_raw, n_mp)
        branch_in, next_mix = second(
            next_raws, coef, bias, scale, sde, branch, gain, features
        )
        return streams_out, branch_in, next_mix.T

    placed = (
        P("dp", None, "mp"),
        P("dp", "mp"),
        P(None, None, ("mp", "dp")),
        P(None, None, ("mp", "dp")),
        P(),
        P(),
        P("mp"),
    )
    return jax.shard_map(
        local,
        mesh=mesh,
        in_specs=placed,
        out_specs=(P("dp", None, "mp"), P("dp", "mp"), P("dp", None)),
        check_vma=False,
    )
```

```python
import functools

import jax
import jax.numpy as jnp
from jax import lax
from jax.experimental import pallas as pl
from jax.experimental.pallas import tpu as pltpu
from jax.sharding import PartitionSpec as P


BALANCE_ROUNDS = 6
EPS = 1e-06
FB = 256
GT = 64
MT = 16
F32 = jnp.float32
BF16 = jnp.bfloat16
MIB = 2**20

VMEM = pl.BlockSpec(memory_space=pltpu.VMEM)
HBM = pl.BlockSpec(memory_space=pltpu.HBM)

RAW_EARLY, RAW_LATE = (0, 1, 2, 3, 4, 6), (5, 7)
PAIRS = [(i, j) for i in range(4) for j in range(i, 4)]


def _nt(a, b, precision=None):
    return lax.dot_general(
        a, b, (((1,), (1,)), ((), ())), precision=precision, preferred_element_type=F32
    )


def _split(x):
    hi = x.astype(BF16)
    return hi, (x - hi.astype(F32)).astype(BF16)


def _iota(shape, dim):
    return lax.broadcasted_iota(jnp.int32, shape, dim)


def _store_by_column(ref, rows, start):
    ref[0:start, :] = rows[0:start]
    for j in range(4):
        for i in range(4):
            source = start + 4 * j + i
            ref[start + 4 * i + j : start + 4 * i + j + 1, :] = rows[source : source + 1]
    if rows.shape[0] > start + 16:
        ref[start + 16 : rows.shape[0], :] = rows[start + 16 :]


def deal_kernel(s_hbm, sil_ref, sde_ref, q_ref, part_ref, sems):
    tokens, _, width = s_hbm.shape
    rows = 4 * GT
    flat = s_hbm.reshape(4 * tokens, width)

    def copy(c):
        return pltpu.make_async_copy(
            flat.at[:, pl.ds(pl.multiple_of(c * 128, 128), 128)], sil_ref.at[c], sems.at[c]
        )

    for c in range(width // 128):
        copy(c).start()
    r, q = _iota((rows, rows), 0), _iota((rows, rows), 1)
    perm = jnp.where(q == 4 * (r % GT) + r // GT, 1.0, 0.0).astype(BF16)
    part_ref[...] = jnp.zeros_like(part_ref)

    def body(k, _):
        copy(2 * k).wait()
        copy(2 * k + 1).wait()
        for g in range(tokens // GT):
            own, mine = pl.ds(g * rows, rows), pl.ds(g * GT, GT)
            x = jnp.concatenate([sil_ref[2 * k, own, :], sil_ref[2 * k + 1, own, :]], axis=1)
            y = jnp.dot(perm, x, preferred_element_type=F32)
            for i in range(4):
                sde_ref[k, i, mine, :] = y[i * GT : (i + 1) * GT].astype(BF16)
            y = y * y
            y = (y[0:GT] + y[GT : 2 * GT]) + (y[2 * GT : 3 * GT] + y[3 * GT :])
            part_ref[mine, :] += y[:, :128] + y[:, 128:]
        return 0

    lax.fori_loop(0, width // FB, body, 0)
    q_ref[...] = jnp.sum(part_ref[...].T.reshape(16, 8, tokens), axis=0)


def deal(streams):
    tokens, _, width = streams.shape
    tiles = width // 128
    return pl.pallas_call(
        deal_kernel,
        out_shape=(
            jax.ShapeDtypeStruct((tiles, 4 * tokens, 128), BF16),
            jax.ShapeDtypeStruct((width // FB, 4, tokens, FB), BF16),
            jax.ShapeDtypeStruct((8, tokens), F32),
        ),
        in_specs=[HBM],
        out_specs=(VMEM, VMEM, VMEM),
        scratch_shapes=[pltpu.VMEM((tokens, 128), F32), pltpu.SemaphoreType.DMA((tiles,))],
        compiler_params=pltpu.CompilerParams(vmem_limit_bytes=20 * MIB),
        cost_estimate=pl.CostEstimate(
            flops=6_000_000_000, bytes_accessed=10 * MIB, transcendentals=0
        ),
        name="deal",
    )(pltpu.with_memory_space_constraint(streams, pltpu.HBM))


def grams_kernel(start, sde_ref, b_ref, g_ref, column_ref):
    blocks, tokens = sde_ref.shape[0], g_ref.shape[1]

    def chunk(c, _):
        at = pl.ds(pl.multiple_of(start + c * 16, 16), 16)
        sums = [None] * 15
        for k in range(blocks):
            for h in range(FB // 128):
                lanes = slice(h * 128, (h + 1) * 128)
                wide = [sde_ref[k, i, at, lanes].astype(F32) for i in range(4)]
                wide.append(b_ref[at, k * FB + h * 128 : k * FB + (h + 1) * 128].astype(F32))
                products = [wide[i] * wide[j] for i, j in PAIRS]
                products += [wide[i] * wide[4] for i in range(5)]
                sums = [p if s is None else s + p for s, p in zip(sums, products)]
        lane = _iota((16, 128), 1)
        column = jnp.zeros((16, 128), F32)
        for p in range(15):
            column = jnp.where(lane == p, jnp.sum(sums[p], axis=1, keepdims=True), column)
        column_ref[pl.ds(pl.multiple_of(c * 16, 16), 16), :] = column
        return 0

    lax.fori_loop(0, tokens // 16, chunk, 0)
    g_ref[...] = column_ref[...].T[0:16]


def grams_of(sde, branch, start, tokens):
    return pl.pallas_call(
        functools.partial(grams_kernel, start),
        out_shape=jax.ShapeDtypeStruct((16, tokens), F32),
        in_specs=[VMEM, VMEM],
        out_specs=VMEM,
        scratch_shapes=[pltpu.VMEM((tokens, 128), F32)],
        compiler_params=pltpu.CompilerParams(vmem_limit_bytes=8 * MIB),
        cost_estimate=pl.CostEstimate(
            flops=3_000_000_000, bytes_accessed=5 * MIB, transcendentals=0
        ),
    )(sde, branch)


def _owner(s, permuted):
    return jnp.bitwise_xor(lax.axis_index("dp"), s) if permuted else s


def raw_kernel(order, permuted, last, *refs):
    count = len(order)
    w_refs, (sde_ref, extra_ref, out_ref, wide_ref, lhs_ref) = refs[:count], refs[count:]
    rows, pad = w_refs[0].shape[0], wide_ref.shape[1]
    wide_ref[...] = jnp.zeros_like(wide_ref)
    total = None
    for n, (s, w_ref) in enumerate(zip(order, w_refs)):
        owner = _owner(s, permuted)
        for i in range(4):
            wide_ref[i, 0:rows, :] = w_ref[:, i, :]
            hi, lo = _split(wide_ref[i])
            lhs_ref[n, i, 0:pad, :] = hi
            lhs_ref[n, i, pad : 2 * pad, :] = lo
            part = _nt(lhs_ref[n, i], sde_ref[owner, i])
            total = part if total is None else total + part
    total = total[0:20] + total[pad : pad + 20]
    if last:
        _store_by_column(out_ref, total + extra_ref[0:20, :], 4)
        out_ref[20:24, :] = extra_ref[20:24, :]
    else:
        out_ref[0:20, :] = total
        out_ref[20:21, :] = jnp.sum(extra_ref[...], axis=0, keepdims=True)
        out_ref[21:24, :] = jnp.zeros((3, total.shape[1]), F32)


def raw(weights, order, sde, extra, permuted, last):
    tokens = sde.shape[2]
    return pl.pallas_call(
        functools.partial(raw_kernel, order, permuted, last),
        out_shape=jax.ShapeDtypeStruct((24, tokens), F32),
        in_specs=[VMEM] * (len(order) + 2),
        out_specs=VMEM,
        scratch_shapes=[
            pltpu.VMEM((4, 32, FB), F32),
            pltpu.VMEM((len(order), 4, 64, FB), BF16),
        ],
        compiler_params=pltpu.CompilerParams(vmem_limit_bytes=12 * MIB),
        cost_estimate=pl.CostEstimate(
            flops=2_000_000_000, bytes_accessed=5 * MIB, transcendentals=0
        ),
    )(*[weights[s] for s in order], sde, extra)


def pair_kernel(*refs):
    w_refs, out_ref = refs[:-1], refs[-1]
    count = w_refs[0].shape[0]
    for s, w_ref in enumerate(w_refs):
        for j in range(4):
            out_ref[s, j * count : (j + 1) * count, :] = w_ref[:, j, :]


def pair(*weights):
    count = weights[0].shape[0]
    return pl.pallas_call(
        pair_kernel,
        out_shape=jax.ShapeDtypeStruct((len(weights), 4 * count, FB), F32),
        in_specs=[VMEM] * len(weights),
        out_specs=VMEM,
        compiler_params=pltpu.CompilerParams(vmem_limit_bytes=4 * MIB),
        cost_estimate=pl.CostEstimate(flops=100_000_000, bytes_accessed=MIB, transcendentals=0),
        name="pair",
    )(*weights)


def _projected(order, permuted, w_refs, sde_ref, b_ref, lhs_ref):
    rows = w_refs[0].shape[1]
    places = [(w_ref, n) for w_ref in w_refs for n in range(w_ref.shape[0])]
    owners = [_owner(s, permuted) for s in order]
    for s, (w_ref, n) in enumerate(places):
        hi, lo = _split(w_ref[n])
        lhs_ref[s, 0:rows, :] = hi
        lhs_ref[s, rows : 2 * rows, :] = lo
    for i in range(5):
        total = None
        for s, owner in enumerate(owners):
            if i < 4:
                right = sde_ref[owner, i]
            else:
                right = b_ref[:, pl.ds(pl.multiple_of(owner * FB, FB), FB)]
            part = _nt(lhs_ref[s], right)
            total = part if total is None else total + part
        yield total[0:rows] + total[rows : 2 * rows]


def early_kernel(order, permuted, *refs):
    w_refs, (sde_ref, b_ref, out_ref, lhs_ref) = refs[:-4], refs[-4:]
    for i, total in enumerate(_projected(order, permuted, w_refs, sde_ref, b_ref, lhs_ref)):
        out_ref[i] = total


def late_kernel(order, permuted, *refs):
    w_refs, refs = refs[:-8], refs[-8:]
    sde_ref, b_ref, early_ref, coef_ref, left_ref, right_ref, out_ref, lhs_ref = refs
    count = w_refs[0].shape[1] // 4
    mixed = None
    for i, total in enumerate(_projected(order, permuted, w_refs, sde_ref, b_ref, lhs_ref)):
        total = total + early_ref[i]
        for j in range(4):
            part = coef_ref[4 * i + j : 4 * i + j + 1, :] * total[j * count : (j + 1) * count]
            mixed = part if mixed is None else mixed + part
    _store_by_column(out_ref, mixed, 8)
    out_ref[count:, :] = jnp.concatenate([left_ref[...], right_ref[...]], axis=1)


def project_early(weights, order, sde, branch, permuted):
    rows, tokens = weights[0].shape[1], sde.shape[2]
    return pl.pallas_call(
        functools.partial(early_kernel, order, permuted),
        out_shape=jax.ShapeDtypeStruct((5, rows, tokens), F32),
        in_specs=[VMEM] * (len(weights) + 2),
        out_specs=VMEM,
        scratch_shapes=[pltpu.VMEM((len(order), 2 * rows, FB), BF16)],
        compiler_params=pltpu.CompilerParams(vmem_limit_bytes=14 * MIB),
        cost_estimate=pl.CostEstimate(
            flops=3_000_000_000, bytes_accessed=6 * MIB, transcendentals=0
        ),
        name="project_early",
    )(*weights, sde, branch)


def project_late(weights, order, sde, branch, early, coef, grams, permuted):
    rows, tokens = weights[0].shape[1], sde.shape[2]
    return pl.pallas_call(
        functools.partial(late_kernel, order, permuted),
        out_shape=jax.ShapeDtypeStruct((rows // 4 + grams[0].shape[0], tokens), F32),
        in_specs=[VMEM] * (len(weights) + 6),
        out_specs=VMEM,
        scratch_shapes=[pltpu.VMEM((len(order), 2 * rows, FB), BF16)],
        compiler_params=pltpu.CompilerParams(vmem_limit_bytes=14 * MIB),
        cost_estimate=pl.CostEstimate(
            flops=3_000_000_000, bytes_accessed=6 * MIB, transcendentals=0
        ),
        name="project_late",
    )(*weights, sde, branch, early, coef, *grams)


def _balance(columns):
    for _ in range(BALANCE_ROUNDS):
        inverse = 1.0 / (columns[0] + columns[1] + columns[2] + columns[3])
        columns = [c * inverse for c in columns]
        columns = [c * (1.0 / jnp.sum(c, axis=0, keepdims=True)) for c in columns]
    return columns


def _sum4(refs, at):
    return (refs[0][at] + refs[1][at]) + (refs[2][at] + refs[3][at])


def _column(ref, start, step):
    wide = ref.shape[1]
    here = _iota((4, wide), 1) == start + step * _iota((4, wide), 0)
    return jnp.sum(jnp.where(here, jnp.broadcast_to(ref[...], (4, wide)), 0.0), axis=1, keepdims=True)


def _scored(raw_rows, inverse, scale, bias):
    return scale * (raw_rows * inverse) + bias


def first_kernel(features, *refs):
    r_refs = refs[0:4]
    bias_ref, scale_ref, coef_ref = refs[4:]
    squares = _sum4(r_refs, (slice(20, 21), slice(None)))
    inverse = 1.0 / jnp.sqrt(squares / features + EPS)
    raw_post = _sum4(r_refs, (slice(0, 4), slice(None)))
    score = _scored(raw_post, inverse, _column(scale_ref, 0, 0), _column(bias_ref, 0, 1))
    coef_ref[16:20, :] = 2.0 * jax.nn.sigmoid(score)
    columns = []
    for i in range(4):
        raw_rows = _sum4(r_refs, (slice(4 + 4 * i, 8 + 4 * i), slice(None)))
        score = _scored(raw_rows, inverse, _column(scale_ref, 1, 0), _column(bias_ref, 4 + i, 4))
        columns.append(jnp.exp(score))
    columns = _balance(columns)
    for i in range(4):
        coef_ref[4 * i : 4 * i + 4, :] = columns[i]
    coef_ref[20:24, :] = jnp.zeros_like(coef_ref[20:24, :])


def first(raws, bias, scale, features):
    tokens = raws[0].shape[1]
    return pl.pallas_call(
        functools.partial(first_kernel, features),
        out_shape=jax.ShapeDtypeStruct((24, tokens), F32),
        in_specs=[VMEM] * 6,
        out_specs=VMEM,
        compiler_params=pltpu.CompilerParams(vmem_limit_bytes=4 * MIB),
        cost_estimate=pl.CostEstimate(
            flops=1_000_000_000, bytes_accessed=MIB, transcendentals=20000
        ),
        name="first",
    )(*raws, bias, scale)


def weave_kernel(coef_ref, left_ref):
    tokens = coef_ref.shape[1]
    rows = 4 * MT
    wide = 2 * rows + 2 * MT
    m, q = _iota((64, wide), 0), _iota((64, wide), 1)
    of_branch = q >= 2 * rows
    low = jnp.where(of_branch, (q - 2 * rows) // MT, q // rows)
    source = jnp.where(of_branch, 4, q % 4)
    pick = jnp.where(m // 4 == low * 8 + source, 1.0, 0.0).astype(BF16)
    r, q = _iota((rows, wide), 0), _iota((rows, wide), 1)
    token = jnp.where(q >= 2 * rows, (q - 2 * rows) % MT, (q % rows) // 4)
    same = token == r // 4
    r, m = _iota((rows, 64), 0), _iota((rows, 64), 1)
    keep = (m % 4) == (r % 4)
    hi, lo = _split(jnp.concatenate([coef_ref[...], jnp.zeros((8, tokens), F32)], axis=0))
    coef = jnp.concatenate([hi, lo], axis=0)
    for g in range(tokens // MT):
        start = g * MT // 128 * 128
        lane, r = _iota((rows, 128), 1), _iota((rows, 128), 0)
        expand = jnp.where(lane == g * MT - start + r // 4, 1.0, 0.0).astype(BF16)
        held = _nt(expand, coef[:, start : start + 128])
        held = jnp.where(keep, held, 0.0).astype(BF16)
        spread = jnp.dot(held, pick, preferred_element_type=F32)
        left_ref[g] = jnp.where(same, spread, 0.0).astype(BF16)


def weave(coef):
    tokens = coef.shape[1]
    return pl.pallas_call(
        weave_kernel,
        out_shape=jax.ShapeDtypeStruct((tokens // MT, 4 * MT, 10 * MT), BF16),
        in_specs=[VMEM],
        out_specs=VMEM,
        compiler_params=pltpu.CompilerParams(vmem_limit_bytes=6 * MIB),
        cost_estimate=pl.CostEstimate(
            flops=1_000_000_000, bytes_accessed=MIB, transcendentals=0
        ),
        name="weave",
    )(coef)


def mix_kernel(left_ref, sil_ref, b_ref, out_hbm, stage_ref, sems):
    tiles, tokens = sil_ref.shape[0], sil_ref.shape[1] // 4
    rows = 4 * MT
    flat = out_hbm.reshape(4 * tokens, tiles * 128)

    def copy(c):
        return pltpu.make_async_copy(
            stage_ref.at[c], flat.at[:, pl.ds(pl.multiple_of(c * 128, 128), 128)], sems.at[c]
        )

    def body(k, _):
        lanes = pl.ds(pl.multiple_of(k * FB, FB), FB)
        for g in range(tokens // MT):
            own = pl.ds(g * rows, rows)
            x = jnp.concatenate([sil_ref[2 * k, own, :], sil_ref[2 * k + 1, own, :]], axis=1)
            b = b_ref[pl.ds(g * MT, MT), lanes]
            right = jnp.concatenate([x, x, b, b], axis=0)
            y = jnp.dot(left_ref[g], right, preferred_element_type=F32)
            y = y.astype(BF16)
            stage_ref[2 * k, own, :] = y[:, :128]
            stage_ref[2 * k + 1, own, :] = y[:, 128:]
        copy(2 * k).start()
        copy(2 * k + 1).start()
        return 0

    lax.fori_loop(0, tiles // 2, body, 0)
    for c in range(tiles):
        copy(c).wait()


def mix(left, sil, branch):
    tiles, tokens = sil.shape[0], sil.shape[1] // 4
    return pl.pallas_call(
        mix_kernel,
        out_shape=jax.ShapeDtypeStruct((tokens, 4, tiles * 128), BF16),
        in_specs=[VMEM, VMEM, VMEM],
        out_specs=HBM,
        scratch_shapes=[
            pltpu.VMEM((tiles, 4 * tokens, 128), BF16),
            pltpu.SemaphoreType.DMA((tiles,)),
        ],
        compiler_params=pltpu.CompilerParams(vmem_limit_bytes=14 * MIB),
        cost_estimate=pl.CostEstimate(
            flops=5_000_000_000, bytes_accessed=8 * MIB, transcendentals=0
        ),
        name="mix",
    )(left, sil, branch)


def second_kernel(features, *refs):
    r_refs = refs[0:4]
    coef_ref, bias_ref, scale_ref, sde_ref, b_ref, gain_ref = refs[4:10]
    out_hbm, mix_hbm, mix_ref, column_ref, w5_ref, out_ref, sems, mix_sem = refs[10:]
    tokens, _ = b_ref.shape
    gram = _sum4(r_refs, (slice(24, 40), slice(None)))
    columns = [coef_ref[4 * i : 4 * i + 4, :] for i in range(5)]

    def quadratic(terms):
        total = None
        for p, (i, j) in enumerate(PAIRS):
            part = terms[i] * terms[j] * gram[p : p + 1]
            part = part if i == j else 2.0 * part
            total = part if total is None else total + part
        for i in range(4):
            total = total + 2.0 * (terms[i] * terms[4]) * gram[10 + i : 11 + i]
        return total + terms[4] * terms[4] * gram[14:15]

    squares = jnp.maximum(jnp.sum(quadratic(columns), axis=0, keepdims=True), 0.0)
    inverse = 1.0 / jnp.sqrt(squares / features + EPS)
    everything = slice(None)
    pre_raw = _sum4(r_refs, (slice(0, 4), everything))
    score = _scored(pre_raw, inverse, _column(scale_ref, 2, 0), _column(bias_ref, 20, 1))
    pre_next = jax.nn.sigmoid(score)
    post_raw = _sum4(r_refs, (slice(4, 8), everything))
    score = _scored(post_raw, inverse, _column(scale_ref, 3, 0), _column(bias_ref, 24, 1))
    mix_ref[0:4, :] = 2.0 * jax.nn.sigmoid(score)
    following = []
    for i in range(4):
        raw_rows = _sum4(r_refs, (slice(8 + 4 * i, 12 + 4 * i), everything))
        score = _scored(raw_rows, inverse, _column(scale_ref, 4, 0), _column(bias_ref, 28 + i, 4))
        following.append(jnp.exp(score))
    following = _balance(following)
    for i in range(4):
        for j in range(4):
            mix_ref[4 + 4 * j + i : 5 + 4 * j + i, :] = following[i][j : j + 1]
    mix_copy = pltpu.make_async_copy(mix_ref, mix_hbm, mix_sem)
    mix_copy.start()

    joint = [jnp.sum(pre_next * c, axis=0, keepdims=True) for c in columns]
    united = jnp.maximum(quadratic(joint), 0.0)
    root = 1.0 / jnp.sqrt(united / (features // 4) + EPS)
    stacked = jnp.concatenate([j * root for j in joint] + [jnp.zeros((3, tokens), F32)], axis=0)
    column_ref[:, 0:8] = stacked.T
    blocks = sde_ref.shape[0]
    for i in range(5):
        w5_ref[i] = jnp.broadcast_to(column_ref[:, i : i + 1], (tokens, 128))

    def copy(c):
        at = pl.ds(pl.multiple_of(c * 32, 32), 32)
        return pltpu.make_async_copy(out_ref.at[at], out_hbm.at[at], sems.at[c])

    def body(c, _):
        for u in range(2):
            at = pl.ds(pl.multiple_of(c * 32 + u * 16, 16), 16)
            weights = [w5_ref[i, at, :] for i in range(5)]
            for k in range(blocks):
                for h in range(FB // 128):
                    part = slice(h * 128, (h + 1) * 128)
                    lanes = slice(k * FB + h * 128, k * FB + (h + 1) * 128)
                    total = weights[4] * b_ref[at, lanes].astype(F32)
                    for i in range(4):
                        total = total + weights[i] * sde_ref[k, i, at, part].astype(F32)
                    out_ref[at, lanes] = (total * gain_ref[:, lanes]).astype(BF16)
        copy(c).start()
        return 0

    lax.fori_loop(0, tokens // 32, body, 0)
    for c in range(tokens // 32):
        copy(c).wait()
    mix_copy.wait()


def second(raws, coef, bias, scale, sde, branch, gain, features):
    tokens, width = branch.shape
    return pl.pallas_call(
        functools.partial(second_kernel, features),
        out_shape=(
            jax.ShapeDtypeStruct((tokens, width), BF16),
            jax.ShapeDtypeStruct((20, tokens), F32),
        ),
        in_specs=[VMEM] * 10,
        out_specs=(HBM, HBM),
        scratch_shapes=[
            pltpu.VMEM((20, tokens), F32),
            pltpu.VMEM((tokens, 128), F32),
            pltpu.VMEM((5, tokens, 128), F32),
            pltpu.VMEM((tokens, width), BF16),
            pltpu.SemaphoreType.DMA((tokens // 16,)),
            pltpu.SemaphoreType.DMA,
        ],
        compiler_params=pltpu.CompilerParams(vmem_limit_bytes=14 * MIB),
        cost_estimate=pl.CostEstimate(
            flops=3_000_000_000, bytes_accessed=6 * MIB, transcendentals=20000
        ),
        name="second",
    )(*raws, coef, bias, scale, sde, branch, gain)


def _swap(x, axis, count, s):
    return lax.ppermute(x, axis, [(i, i ^ s) for i in range(count)])


def by_block(weight, width):
    whole = lax.all_gather(weight, "dp", axis=2, tiled=True)
    return [whole[:, :, k * FB : (k + 1) * FB] for k in range(width // FB)]


def gather_merge(weight, count, width):
    if count != 8 or count * weight.shape[2] != width or weight.shape[2] != FB:
        return by_block(weight, width), False
    blocks = {0: weight}
    for s in (2, 4, 6):
        blocks[s] = _swap(weight, "dp", count, s)
    for s in (0, 2, 4, 6):
        blocks[s + 1] = _swap(blocks[s], "dp", count, 1)
    return [blocks[s] for s in range(count)], True


def gather_next(weight, count, width):
    if count != 8 or count * weight.shape[2] != width or weight.shape[2] != FB:
        blocks = by_block(weight, width)
        return [pair(*blocks[:-2]), pair(*blocks[-2:])], tuple(range(width // FB))
    far = _swap(weight, "dp", count, 2)
    here = pair(weight, far)
    there = _swap(here, "dp", count, 4)
    near = _swap(here, "dp", count, 1)
    across = _swap(there, "dp", count, 1)
    return [here, near, there, across], (0, 2, 1, 3, 4, 6, 5, 7)


def everyone(x, count):
    return [x] + [_swap(x, "mp", count, s) for s in range(1, count)]


def solution(mesh):
    n_dp, n_mp = mesh.shape["dp"], mesh.shape["mp"]

    def local(streams, branch, merge_weight, next_weight, blend_bias, blend_scale, norm_gain):
        count, width = streams.shape[1:]
        features = count * width * n_mp
        tokens = streams.shape[0]
        merge_blocks, permuted = gather_merge(merge_weight, n_dp, width)
        next_blocks, order = gather_next(next_weight, n_dp, width)
        gain, bias, scale = norm_gain[None, :], blend_bias[None, :], blend_scale[None, :]
        sil, sde, squares = deal(streams)
        part = raw(merge_blocks, RAW_EARLY, sde, squares, permuted, False)
        part = raw(merge_blocks, RAW_LATE, sde, part, permuted, True)
        raws = everyone(part, n_mp)
        half = tokens // 2
        grams = [grams_of(sde, branch, 0, half), grams_of(sde, branch, half, tokens - half)]
        coef = first(raws, bias, scale, features)
        streams_out = mix(weave(coef), sil, branch)
        early = project_early(next_blocks[:-1], order[:-2], sde, branch, permuted)
        next_raw = project_late(
            next_blocks[-1:], order[-2:], sde, branch, early, coef, grams, permuted
        )
        next_raws = everyone(next_raw, n_mp)
        branch_in, next_mix = second(
            next_raws, coef, bias, scale, sde, branch, gain, features
        )
        return streams_out, branch_in, next_mix.T

    placed = (
        P("dp", None, "mp"),
        P("dp", "mp"),
        P(None, None, ("mp", "dp")),
        P(None, None, ("mp", "dp")),
        P(),
        P(),
        P("mp"),
    )
    return jax.shard_map(
        local,
        mesh=mesh,
        in_specs=placed,
        out_specs=(P("dp", None, "mp"), P("dp", "mp"), P("dp", None)),
        check_vma=False,
    )
```

```python
import functools

import jax
import jax.numpy as jnp
from jax import lax
from jax.experimental import pallas as pl
from jax.experimental.pallas import tpu as pltpu
from jax.sharding import PartitionSpec as P


BALANCE_ROUNDS = 6
EPS = 1e-06
FB = 256
GT = 64
MT = 16
F32 = jnp.float32
BF16 = jnp.bfloat16
MIB = 2**20

VMEM = pl.BlockSpec(memory_space=pltpu.VMEM)
HBM = pl.BlockSpec(memory_space=pltpu.HBM)

RAW_EARLY, RAW_LATE = (0, 1, 2, 3, 4, 6), (5, 7)
PAIRS = [(i, j) for i in range(4) for j in range(i, 4)]


def _nt(a, b, precision=None):
    return lax.dot_general(
        a, b, (((1,), (1,)), ((), ())), precision=precision, preferred_element_type=F32
    )


def _split(x):
    hi = x.astype(BF16)
    return hi, (x - hi.astype(F32)).astype(BF16)


def _iota(shape, dim):
    return lax.broadcasted_iota(jnp.int32, shape, dim)


def _store_by_column(ref, rows, start):
    ref[0:start, :] = rows[0:start]
    for j in range(4):
        for i in range(4):
            source = start + 4 * j + i
            ref[start + 4 * i + j : start + 4 * i + j + 1, :] = rows[source : source + 1]
    if rows.shape[0] > start + 16:
        ref[start + 16 : rows.shape[0], :] = rows[start + 16 :]


def deal_kernel(s_hbm, sil_ref, sde_ref, q_ref, part_ref, sems):
    tokens, _, width = s_hbm.shape
    rows = 4 * GT
    flat = s_hbm.reshape(4 * tokens, width)

    def copy(c):
        return pltpu.make_async_copy(
            flat.at[:, pl.ds(pl.multiple_of(c * 128, 128), 128)], sil_ref.at[c], sems.at[c]
        )

    for c in range(width // 128):
        copy(c).start()
    r, q = _iota((rows, rows), 0), _iota((rows, rows), 1)
    perm = jnp.where(q == 4 * (r % GT) + r // GT, 1.0, 0.0).astype(BF16)
    part_ref[...] = jnp.zeros_like(part_ref)

    def body(k, _):
        copy(2 * k).wait()
        copy(2 * k + 1).wait()
        for g in range(tokens // GT):
            own, mine = pl.ds(g * rows, rows), pl.ds(g * GT, GT)
            x = jnp.concatenate([sil_ref[2 * k, own, :], sil_ref[2 * k + 1, own, :]], axis=1)
            y = jnp.dot(perm, x, preferred_element_type=F32)
            for i in range(4):
                sde_ref[k, i, mine, :] = y[i * GT : (i + 1) * GT].astype(BF16)
            y = y * y
            y = (y[0:GT] + y[GT : 2 * GT]) + (y[2 * GT : 3 * GT] + y[3 * GT :])
            part_ref[mine, :] += y[:, :128] + y[:, 128:]
        return 0

    lax.fori_loop(0, width // FB, body, 0)
    q_ref[...] = jnp.sum(part_ref[...].T.reshape(16, 8, tokens), axis=0)


def deal(streams):
    tokens, _, width = streams.shape
    tiles = width // 128
    return pl.pallas_call(
        deal_kernel,
        out_shape=(
            jax.ShapeDtypeStruct((tiles, 4 * tokens, 128), BF16),
            jax.ShapeDtypeStruct((width // FB, 4, tokens, FB), BF16),
            jax.ShapeDtypeStruct((8, tokens), F32),
        ),
        in_specs=[HBM],
        out_specs=(VMEM, VMEM, VMEM),
        scratch_shapes=[pltpu.VMEM((tokens, 128), F32), pltpu.SemaphoreType.DMA((tiles,))],
        compiler_params=pltpu.CompilerParams(vmem_limit_bytes=20 * MIB),
        cost_estimate=pl.CostEstimate(
            flops=6_000_000_000, bytes_accessed=10 * MIB, transcendentals=0
        ),
        name="deal",
    )(pltpu.with_memory_space_constraint(streams, pltpu.HBM))


def grams_kernel(start, sde_ref, b_ref, g_ref, column_ref):
    blocks, tokens = sde_ref.shape[0], g_ref.shape[1]

    def chunk(c, _):
        at = pl.ds(pl.multiple_of(start + c * 16, 16), 16)
        sums = [None] * 15
        for k in range(blocks):
            for h in range(FB // 128):
                lanes = slice(h * 128, (h + 1) * 128)
                wide = [sde_ref[k, i, at, lanes].astype(F32) for i in range(4)]
                wide.append(b_ref[at, k * FB + h * 128 : k * FB + (h + 1) * 128].astype(F32))
                products = [wide[i] * wide[j] for i, j in PAIRS]
                products += [wide[i] * wide[4] for i in range(5)]
                sums = [p if s is None else s + p for s, p in zip(sums, products)]
        lane = _iota((16, 128), 1)
        column = jnp.zeros((16, 128), F32)
        for p in range(15):
            column = jnp.where(lane == p, jnp.sum(sums[p], axis=1, keepdims=True), column)
        column_ref[pl.ds(pl.multiple_of(c * 16, 16), 16), :] = column
        return 0

    lax.fori_loop(0, tokens // 16, chunk, 0)
    g_ref[...] = column_ref[...].T[0:16]


def grams_of(sde, branch, start, tokens):
    return pl.pallas_call(
        functools.partial(grams_kernel, start),
        out_shape=jax.ShapeDtypeStruct((16, tokens), F32),
        in_specs=[VMEM, VMEM],
        out_specs=VMEM,
        scratch_shapes=[pltpu.VMEM((tokens, 128), F32)],
        compiler_params=pltpu.CompilerParams(vmem_limit_bytes=8 * MIB),
        cost_estimate=pl.CostEstimate(
            flops=3_000_000_000, bytes_accessed=5 * MIB, transcendentals=0
        ),
    )(sde, branch)


def _owner(s, permuted):
    return jnp.bitwise_xor(lax.axis_index("dp"), s) if permuted else s


def raw_kernel(order, permuted, last, *refs):
    count = len(order)
    w_refs, (sde_ref, extra_ref, out_ref, wide_ref, lhs_ref) = refs[:count], refs[count:]
    rows, pad = w_refs[0].shape[0], wide_ref.shape[1]
    wide_ref[...] = jnp.zeros_like(wide_ref)
    total = None
    for n, (s, w_ref) in enumerate(zip(order, w_refs)):
        owner = _owner(s, permuted)
        for i in range(4):
            wide_ref[i, 0:rows, :] = w_ref[:, i, :]
            hi, lo = _split(wide_ref[i])
            lhs_ref[n, i, 0:pad, :] = hi
            lhs_ref[n, i, pad : 2 * pad, :] = lo
            part = _nt(lhs_ref[n, i], sde_ref[owner, i])
            total = part if total is None else total + part
    total = total[0:20] + total[pad : pad + 20]
    if last:
        _store_by_column(out_ref, total + extra_ref[0:20, :], 4)
        out_ref[20:24, :] = extra_ref[20:24, :]
    else:
        out_ref[0:20, :] = total
        out_ref[20:21, :] = jnp.sum(extra_ref[...], axis=0, keepdims=True)
        out_ref[21:24, :] = jnp.zeros((3, total.shape[1]), F32)


def raw(weights, order, sde, extra, permuted, last):
    tokens = sde.shape[2]
    return pl.pallas_call(
        functools.partial(raw_kernel, order, permuted, last),
        out_shape=jax.ShapeDtypeStruct((24, tokens), F32),
        in_specs=[VMEM] * (len(order) + 2),
        out_specs=VMEM,
        scratch_shapes=[
            pltpu.VMEM((4, 32, FB), F32),
            pltpu.VMEM((len(order), 4, 64, FB), BF16),
        ],
        compiler_params=pltpu.CompilerParams(vmem_limit_bytes=12 * MIB),
        cost_estimate=pl.CostEstimate(
            flops=2_000_000_000, bytes_accessed=5 * MIB, transcendentals=0
        ),
    )(*[weights[s] for s in order], sde, extra)


def pair_kernel(*refs):
    w_refs, out_ref = refs[:-1], refs[-1]
    count = w_refs[0].shape[0]
    for s, w_ref in enumerate(w_refs):
        for j in range(4):
            out_ref[s, j * count : (j + 1) * count, :] = w_ref[:, j, :]


def pair(*weights):
    count = weights[0].shape[0]
    return pl.pallas_call(
        pair_kernel,
        out_shape=jax.ShapeDtypeStruct((len(weights), 4 * count, FB), F32),
        in_specs=[VMEM] * len(weights),
        out_specs=VMEM,
        compiler_params=pltpu.CompilerParams(vmem_limit_bytes=4 * MIB),
        cost_estimate=pl.CostEstimate(flops=100_000_000, bytes_accessed=MIB, transcendentals=0),
        name="pair",
    )(*weights)


def _projected(order, permuted, w_refs, sde_ref, b_ref, lhs_ref):
    rows = w_refs[0].shape[1]
    places = [(w_ref, n) for w_ref in w_refs for n in range(w_ref.shape[0])]
    owners = [_owner(s, permuted) for s in order]
    for s, (w_ref, n) in enumerate(places):
        hi, lo = _split(w_ref[n])
        lhs_ref[s, 0:rows, :] = hi
        lhs_ref[s, rows : 2 * rows, :] = lo
    for i in range(5):
        total = None
        for s, owner in enumerate(owners):
            if i < 4:
                right = sde_ref[owner, i]
            else:
                right = b_ref[:, pl.ds(pl.multiple_of(owner * FB, FB), FB)]
            part = _nt(lhs_ref[s], right)
            total = part if total is None else total + part
        yield total[0:rows] + total[rows : 2 * rows]


def early_kernel(order, permuted, *refs):
    w_refs, (sde_ref, b_ref, out_ref, lhs_ref) = refs[:-4], refs[-4:]
    for i, total in enumerate(_projected(order, permuted, w_refs, sde_ref, b_ref, lhs_ref)):
        out_ref[i] = total


def late_kernel(order, permuted, *refs):
    w_refs, refs = refs[:-8], refs[-8:]
    sde_ref, b_ref, early_ref, coef_ref, left_ref, right_ref, out_ref, lhs_ref = refs
    count = w_refs[0].shape[1] // 4
    mixed = None
    for i, total in enumerate(_projected(order, permuted, w_refs, sde_ref, b_ref, lhs_ref)):
        total = total + early_ref[i]
        for j in range(4):
            part = coef_ref[4 * i + j : 4 * i + j + 1, :] * total[j * count : (j + 1) * count]
            mixed = part if mixed is None else mixed + part
    _store_by_column(out_ref, mixed, 8)
    out_ref[count:, :] = jnp.concatenate([left_ref[...], right_ref[...]], axis=1)


def project_early(weights, order, sde, branch, permuted):
    rows, tokens = weights[0].shape[1], sde.shape[2]
    return pl.pallas_call(
        functools.partial(early_kernel, order, permuted),
        out_shape=jax.ShapeDtypeStruct((5, rows, tokens), F32),
        in_specs=[VMEM] * (len(weights) + 2),
        out_specs=VMEM,
        scratch_shapes=[pltpu.VMEM((len(order), 2 * rows, FB), BF16)],
        compiler_params=pltpu.CompilerParams(vmem_limit_bytes=14 * MIB),
        cost_estimate=pl.CostEstimate(
            flops=3_000_000_000, bytes_accessed=6 * MIB, transcendentals=0
        ),
        name="project_early",
    )(*weights, sde, branch)


def project_late(weights, order, sde, branch, early, coef, grams, permuted):
    rows, tokens = weights[0].shape[1], sde.shape[2]
    return pl.pallas_call(
        functools.partial(late_kernel, order, permuted),
        out_shape=jax.ShapeDtypeStruct((rows // 4 + grams[0].shape[0], tokens), F32),
        in_specs=[VMEM] * (len(weights) + 6),
        out_specs=VMEM,
        scratch_shapes=[pltpu.VMEM((len(order), 2 * rows, FB), BF16)],
        compiler_params=pltpu.CompilerParams(vmem_limit_bytes=14 * MIB),
        cost_estimate=pl.CostEstimate(
            flops=3_000_000_000, bytes_accessed=6 * MIB, transcendentals=0
        ),
        name="project_late",
    )(*weights, sde, branch, early, coef, *grams)


def _balance(columns):
    for turn in range(BALANCE_ROUNDS):
        total = columns[0] + columns[1] + columns[2] + columns[3]
        if turn == 0:
            columns = [c / total for c in columns]
        else:
            inverse = 1.0 / total
            columns = [c * inverse for c in columns]
        columns = [c * (1.0 / jnp.sum(c, axis=0, keepdims=True)) for c in columns]
    return columns


def _sum4(refs, at):
    return (refs[0][at] + refs[1][at]) + (refs[2][at] + refs[3][at])


def _column(ref, start, step):
    wide = ref.shape[1]
    here = _iota((4, wide), 1) == start + step * _iota((4, wide), 0)
    return jnp.sum(jnp.where(here, jnp.broadcast_to(ref[...], (4, wide)), 0.0), axis=1, keepdims=True)


def _scored(raw_rows, inverse, scale, bias):
    return scale * (raw_rows * inverse) + bias


def first_kernel(features, *refs):
    r_refs = refs[0:4]
    bias_ref, scale_ref, coef_ref = refs[4:]
    squares = _sum4(r_refs, (slice(20, 21), slice(None)))
    inverse = 1.0 / jnp.sqrt(squares / features + EPS)
    raw_post = _sum4(r_refs, (slice(0, 4), slice(None)))
    score = _scored(raw_post, inverse, _column(scale_ref, 0, 0), _column(bias_ref, 0, 1))
    coef_ref[16:20, :] = 2.0 * jax.nn.sigmoid(score)
    columns = []
    for i in range(4):
        raw_rows = _sum4(r_refs, (slice(4 + 4 * i, 8 + 4 * i), slice(None)))
        score = _scored(raw_rows, inverse, _column(scale_ref, 1, 0), _column(bias_ref, 4 + i, 4))
        columns.append(jnp.exp(score))
    columns = _balance(columns)
    for i in range(4):
        coef_ref[4 * i : 4 * i + 4, :] = columns[i]
    coef_ref[20:24, :] = jnp.zeros_like(coef_ref[20:24, :])


def first(raws, bias, scale, features):
    tokens = raws[0].shape[1]
    return pl.pallas_call(
        functools.partial(first_kernel, features),
        out_shape=jax.ShapeDtypeStruct((24, tokens), F32),
        in_specs=[VMEM] * 6,
        out_specs=VMEM,
        compiler_params=pltpu.CompilerParams(vmem_limit_bytes=4 * MIB),
        cost_estimate=pl.CostEstimate(
            flops=1_000_000_000, bytes_accessed=MIB, transcendentals=20000
        ),
        name="first",
    )(*raws, bias, scale)


def weave_kernel(coef_ref, left_ref):
    tokens = coef_ref.shape[1]
    rows = 4 * MT
    wide = 2 * rows + 2 * MT
    m, q = _iota((64, wide), 0), _iota((64, wide), 1)
    of_branch = q >= 2 * rows
    low = jnp.where(of_branch, (q - 2 * rows) // MT, q // rows)
    source = jnp.where(of_branch, 4, q % 4)
    pick = jnp.where(m // 4 == low * 8 + source, 1.0, 0.0).astype(BF16)
    half = min(tokens, 128)
    r, q = _iota((4 * half, wide), 0), _iota((4 * half, wide), 1)
    token = jnp.where(q >= 2 * rows, (q - 2 * rows) % MT, (q % rows) // 4)
    same = token == (r // 4) % MT
    r, m = _iota((4 * half, 64), 0), _iota((4 * half, 64), 1)
    keep = (m % 4) == (r % 4)
    r, lane = _iota((4 * half, half), 0), _iota((4 * half, half), 1)
    expand = jnp.where(lane == r // 4, 1.0, 0.0).astype(BF16)
    hi, lo = _split(jnp.concatenate([coef_ref[...], jnp.zeros((8, tokens), F32)], axis=0))
    coef = jnp.concatenate([hi, lo], axis=0)
    for h in range(tokens // half):
        held = _nt(expand, coef[:, h * half : (h + 1) * half])
        held = jnp.where(keep, held, 0.0).astype(BF16)
        spread = jnp.dot(held, pick, preferred_element_type=F32)
        spread = jnp.where(same, spread, 0.0).astype(BF16)
        for g in range(half // MT):
            left_ref[h * (half // MT) + g] = spread[g * rows : (g + 1) * rows]


def weave(coef):
    tokens = coef.shape[1]
    return pl.pallas_call(
        weave_kernel,
        out_shape=jax.ShapeDtypeStruct((tokens // MT, 4 * MT, 10 * MT), BF16),
        in_specs=[VMEM],
        out_specs=VMEM,
        compiler_params=pltpu.CompilerParams(vmem_limit_bytes=6 * MIB),
        cost_estimate=pl.CostEstimate(
            flops=1_000_000_000, bytes_accessed=MIB, transcendentals=0
        ),
        name="weave",
    )(coef)


def mix_kernel(start, stop, left_ref, sil_ref, b_ref, *refs):
    out_hbm, stage_ref, sems = refs[-3:]
    tiles, tokens = sil_ref.shape[0], sil_ref.shape[1] // 4
    rows = 4 * MT
    flat = out_hbm.reshape(4 * tokens, tiles * 128)

    def copy(c):
        return pltpu.make_async_copy(
            stage_ref.at[c], flat.at[:, pl.ds(pl.multiple_of(c * 128, 128), 128)], sems.at[c]
        )

    def body(k, _):
        lanes = pl.ds(pl.multiple_of(k * FB, FB), FB)
        for g in range(tokens // MT):
            own = pl.ds(g * rows, rows)
            x = jnp.concatenate([sil_ref[2 * k, own, :], sil_ref[2 * k + 1, own, :]], axis=1)
            b = b_ref[pl.ds(g * MT, MT), lanes]
            right = jnp.concatenate([x, x, b, b], axis=0)
            y = jnp.dot(left_ref[g], right, preferred_element_type=F32)
            y = y.astype(BF16)
            stage_ref[2 * k, own, :] = y[:, :128]
            stage_ref[2 * k + 1, own, :] = y[:, 128:]
        copy(2 * k).start()
        copy(2 * k + 1).start()
        return 0

    lax.fori_loop(start, stop, body, 0)
    for c in range(2 * start, 2 * stop):
        copy(c).wait()


def mix(left, sil, branch, start, stop, merged):
    tiles, tokens = sil.shape[0], branch.shape[0]
    before = [] if merged is None else [merged]
    return pl.pallas_call(
        functools.partial(mix_kernel, start, stop),
        out_shape=jax.ShapeDtypeStruct((tokens, 4, tiles * 128), BF16),
        in_specs=[VMEM, VMEM, VMEM] + [HBM] * len(before),
        out_specs=HBM,
        scratch_shapes=[
            pltpu.VMEM((tiles, 4 * tokens, 128), BF16),
            pltpu.SemaphoreType.DMA((tiles,)),
        ],
        input_output_aliases={3: 0} if before else {},
        compiler_params=pltpu.CompilerParams(vmem_limit_bytes=14 * MIB),
        cost_estimate=pl.CostEstimate(
            flops=2_000_000_000, bytes_accessed=4 * MIB, transcendentals=0
        ),
    )(left, sil, branch, *before)


def second_kernel(features, *refs):
    r_refs = refs[0:4]
    coef_ref, bias_ref, scale_ref, sde_ref, b_ref, gain_ref = refs[4:10]
    out_hbm, mix_hbm, mix_ref, column_ref, w5_ref, out_ref, sems, mix_sem = refs[10:]
    tokens, _ = b_ref.shape
    gram = _sum4(r_refs, (slice(24, 40), slice(None)))
    columns = [coef_ref[4 * i : 4 * i + 4, :] for i in range(5)]

    def quadratic(terms):
        total = None
        for p, (i, j) in enumerate(PAIRS):
            part = terms[i] * terms[j] * gram[p : p + 1]
            part = part if i == j else 2.0 * part
            total = part if total is None else total + part
        for i in range(4):
            total = total + 2.0 * (terms[i] * terms[4]) * gram[10 + i : 11 + i]
        return total + terms[4] * terms[4] * gram[14:15]

    squares = jnp.maximum(jnp.sum(quadratic(columns), axis=0, keepdims=True), 0.0)
    inverse = 1.0 / jnp.sqrt(squares / features + EPS)
    everything = slice(None)
    pre_raw = _sum4(r_refs, (slice(0, 4), everything))
    score = _scored(pre_raw, inverse, _column(scale_ref, 2, 0), _column(bias_ref, 20, 1))
    pre_next = jax.nn.sigmoid(score)
    post_raw = _sum4(r_refs, (slice(4, 8), everything))
    score = _scored(post_raw, inverse, _column(scale_ref, 3, 0), _column(bias_ref, 24, 1))
    mix_ref[0:4, :] = 2.0 * jax.nn.sigmoid(score)
    following = []
    for i in range(4):
        raw_rows = _sum4(r_refs, (slice(8 + 4 * i, 12 + 4 * i), everything))
        score = _scored(raw_rows, inverse, _column(scale_ref, 4, 0), _column(bias_ref, 28 + i, 4))
        following.append(jnp.exp(score))
    following = _balance(following)
    for i in range(4):
        for j in range(4):
            mix_ref[4 + 4 * j + i : 5 + 4 * j + i, :] = following[i][j : j + 1]
    mix_copy = pltpu.make_async_copy(mix_ref, mix_hbm, mix_sem)
    mix_copy.start()

    joint = [jnp.sum(pre_next * c, axis=0, keepdims=True) for c in columns]
    united = jnp.maximum(quadratic(joint), 0.0)
    root = 1.0 / jnp.sqrt(united / (features // 4) + EPS)
    stacked = jnp.concatenate([j * root for j in joint] + [jnp.zeros((3, tokens), F32)], axis=0)
    column_ref[:, 0:8] = stacked.T
    blocks = sde_ref.shape[0]
    for i in range(5):
        w5_ref[i] = jnp.broadcast_to(column_ref[:, i : i + 1], (tokens, 128))

    def copy(c):
        at = pl.ds(pl.multiple_of(c * 32, 32), 32)
        return pltpu.make_async_copy(out_ref.at[at], out_hbm.at[at], sems.at[c])

    def body(c, _):
        for u in range(2):
            at = pl.ds(pl.multiple_of(c * 32 + u * 16, 16), 16)
            weights = [w5_ref[i, at, :] for i in range(5)]
            for k in range(blocks):
                for h in range(FB // 128):
                    part = slice(h * 128, (h + 1) * 128)
                    lanes = slice(k * FB + h * 128, k * FB + (h + 1) * 128)
                    total = weights[4] * b_ref[at, lanes].astype(F32)
                    for i in range(4):
                        total = total + weights[i] * sde_ref[k, i, at, part].astype(F32)
                    out_ref[at, lanes] = (total * gain_ref[:, lanes]).astype(BF16)
        copy(c).start()
        return 0

    lax.fori_loop(0, tokens // 32, body, 0)
    for c in range(tokens // 32):
        copy(c).wait()
    mix_copy.wait()


def second(raws, coef, bias, scale, sde, branch, gain, features):
    tokens, width = branch.shape
    return pl.pallas_call(
        functools.partial(second_kernel, features),
        out_shape=(
            jax.ShapeDtypeStruct((tokens, width), BF16),
            jax.ShapeDtypeStruct((20, tokens), F32),
        ),
        in_specs=[VMEM] * 10,
        out_specs=(HBM, HBM),
        scratch_shapes=[
            pltpu.VMEM((20, tokens), F32),
            pltpu.VMEM((tokens, 128), F32),
            pltpu.VMEM((5, tokens, 128), F32),
            pltpu.VMEM((tokens, width), BF16),
            pltpu.SemaphoreType.DMA((tokens // 16,)),
            pltpu.SemaphoreType.DMA,
        ],
        compiler_params=pltpu.CompilerParams(vmem_limit_bytes=14 * MIB),
        cost_estimate=pl.CostEstimate(
            flops=3_000_000_000, bytes_accessed=6 * MIB, transcendentals=20000
        ),
        name="second",
    )(*raws, coef, bias, scale, sde, branch, gain)


def _swap(x, axis, count, s):
    return lax.ppermute(x, axis, [(i, i ^ s) for i in range(count)])


def by_block(weight, width):
    whole = lax.all_gather(weight, "dp", axis=2, tiled=True)
    return [whole[:, :, k * FB : (k + 1) * FB] for k in range(width // FB)]


def gather_merge(weight, count, width):
    if count != 8 or count * weight.shape[2] != width or weight.shape[2] != FB:
        return by_block(weight, width), False
    blocks = {0: weight}
    for s in (2, 4, 6):
        blocks[s] = _swap(weight, "dp", count, s)
    for s in (0, 2, 4, 6):
        blocks[s + 1] = _swap(blocks[s], "dp", count, 1)
    return [blocks[s] for s in range(count)], True


def gather_next(weight, count, width):
    if count != 8 or count * weight.shape[2] != width or weight.shape[2] != FB:
        blocks = by_block(weight, width)
        return [pair(*blocks[:-2]), pair(*blocks[-2:])], tuple(range(width // FB))
    far = _swap(weight, "dp", count, 2)
    here = pair(weight, far)
    there = _swap(here, "dp", count, 4)
    near = _swap(here, "dp", count, 1)
    across = _swap(there, "dp", count, 1)
    return [here, near, there, across], (0, 2, 1, 3, 4, 6, 5, 7)


def everyone(x, count):
    return [x] + [_swap(x, "mp", count, s) for s in range(1, count)]


def solution(mesh):
    n_dp, n_mp = mesh.shape["dp"], mesh.shape["mp"]

    def local(streams, branch, merge_weight, next_weight, blend_bias, blend_scale, norm_gain):
        count, width = streams.shape[1:]
        features = count * width * n_mp
        tokens = streams.shape[0]
        merge_blocks, permuted = gather_merge(merge_weight, n_dp, width)
        next_blocks, order = gather_next(next_weight, n_dp, width)
        gain, bias, scale = norm_gain[None, :], blend_bias[None, :], blend_scale[None, :]
        sil, sde, squares = deal(streams)
        part = raw(merge_blocks, RAW_EARLY, sde, squares, permuted, False)
        part = raw(merge_blocks, RAW_LATE, sde, part, permuted, True)
        raws = everyone(part, n_mp)
        half = tokens // 2
        grams = [grams_of(sde, branch, 0, half), grams_of(sde, branch, half, tokens - half)]
        coef = first(raws, bias, scale, features)
        left = weave(coef)
        blocks = width // FB
        merged = mix(left, sil, branch, 0, blocks // 4, None)
        streams_out = mix(left, sil, branch, blocks // 4, blocks, merged)
        early = project_early(next_blocks[:-1], order[:-2], sde, branch, permuted)
        next_raw = project_late(
            next_blocks[-1:], order[-2:], sde, branch, early, coef, grams, permuted
        )
        next_raws = everyone(next_raw, n_mp)
        branch_in, next_mix = second(
            next_raws, coef, bias, scale, sde, branch, gain, features
        )
        return streams_out, branch_in, next_mix.T

    placed = (
        P("dp", None, "mp"),
        P("dp", "mp"),
        P(None, None, ("mp", "dp")),
        P(None, None, ("mp", "dp")),
        P(),
        P(),
        P("mp"),
    )
    return jax.shard_map(
        local,
        mesh=mesh,
        in_specs=placed,
        out_specs=(P("dp", None, "mp"), P("dp", "mp"), P("dp", None)),
        check_vma=False,
    )
```
